256 devices in a mesh: clips: 2 (over z), tm: 16 (over y, core), height: 8 (over x).
Axes of the slice: x: 8, y: 8, z: 2, core: 2. Of those that a mesh axis runs over, the one named last changes fastest.
The devices are a block of a 8x8x16 slice.
Arguments:
- features: bfloat16 [64, 32, 96, 512], P(('clips', 'tm'), 'height'), parts along dimension 0, may hold values from -1000 to 1000
- gain: float32 [512], replicated, may hold values from 0.1 to 1.9
- shift: float32 [512], replicated, may hold values from -3 to 3
- kernel: bfloat16 [3, 3, 3, 512, 256], replicated, may hold values from -0.0546875 to 0.0546875
- bias: float32 [256], replicated, may hold values from -3 to 3
Outputs:
- decoded: bfloat16 [64, 32, 96, 256], P(('clips', 'tm'), 'height'), parts along dimension 0
The draws below stay inside these ranges and needn't reach their ends.
There are 2 independent parts, one for each index of `clips`. The reference program is written for one: setup_inputs(seed, part) draws one part's arguments, and reference() takes and returns one part's arrays. A program takes and returns all parts, laid end to end along the dimension named above; an argument that names none is the same for every part. Nothing has to cross between parts.
All inputs are finite; a program needn't handle non-finite values.
Results may differ from the reference program's by a relative error of at most 0.0055.
Values may be sent and summed in bfloat16 or wider, within the bound.
A program may use at most 64 MiB of HBM per device.

```python
import jax
import jax.numpy as jnp
from jax import lax

CHANNELS = 512
COUT = 256
GROUPS = 32
COLS = 96
FRAMES = 32
ROWS = 32


def draw_features(key, part):
    keys = jax.random.split(jax.random.fold_in(key, 17), 5)
    frame_pos = jnp.arange(FRAMES, dtype=jnp.float32) / max(FRAMES - 1, 1)
    frame_trend = jnp.exp(jnp.log(3.0) * frame_pos)
    chan_scale = jnp.exp(jax.random.uniform(keys[1], (CHANNELS,), jnp.float32, 0.0, jnp.log(10.0)))
    chan_offset = 0.5 * jax.random.normal(keys[2], (CHANNELS,), jnp.float32)
    noise = jnp.clip(jax.random.normal(keys[0], (FRAMES, ROWS, COLS, CHANNELS), jnp.float32), -6.0, 6.0)
    frame_random = jnp.exp(jax.random.uniform(keys[4], (FRAMES,), jnp.float32, -jnp.log(2.0), jnp.log(2.0)))
    frame_scale = frame_trend * frame_random
    values = (noise + chan_offset) * chan_scale
    values = values * frame_scale[:, None, None, None]
    values = jnp.clip(values, -1000.0, 1000.0)
    return values.astype(jnp.bfloat16)


def bell_draw(stream_key, extent, deviation, reach, held_as=jnp.bfloat16):
    result = deviation * jax.random.normal(stream_key, extent, jnp.float32)
    return jnp.clip(result, min=-reach, max=reach).astype(held_as)


def setup_inputs(seed: int = 0, part: int = 0) -> dict:
    key_list = jax.random.split(jax.random.key(seed), 6)
    part_splits = jax.random.split(jax.random.fold_in(key_list[5], part), 6)
    features = draw_features(jax.random.fold_in(jax.random.fold_in(key_list[5], part), 71), part)
    gain = jnp.clip(1.0 + 0.18 * jax.random.normal(key_list[1], (CHANNELS,), jnp.float32), 0.1, 1.9)
    shift = bell_draw(key_list[2], (CHANNELS,), 0.5, 3.0, jnp.float32)
    kernel = bell_draw(key_list[3], (3, 3, 3, CHANNELS, COUT), (27 * CHANNELS) ** -0.5, 0.0546875)
    bias = bell_draw(key_list[4], (COUT,), 0.5, 3.0, jnp.float32)
    return {"features": features, "gain": gain, "shift": shift, "kernel": kernel, "bias": bias}


epsilon = 1e-06

def reference(features, gain, shift, kernel, bias):
    per_group = CHANNELS // GROUPS
    wide_values = features.astype(jnp.float32).reshape(FRAMES, ROWS, COLS, GROUPS, per_group)
    cells_total = FRAMES * ROWS * COLS * per_group
    group_mean = lax.optimization_barrier(jnp.sum(wide_values, axis=(0, 1, 2, 4))) / cells_total
    centered = wide_values - group_mean[:, None]
    group_var = lax.optimization_barrier(jnp.sum(centered * centered, axis=(0, 1, 2, 4))) / cells_total
    normed = centered * lax.rsqrt(group_var + epsilon)[:, None]
    normed = normed.reshape(FRAMES, ROWS, COLS, CHANNELS) * gain + shift
    activated = jax.nn.silu(normed).astype(jnp.bfloat16)
    padded = jnp.concatenate([activated[:1], activated[:1], activated], 0)
    padded = jnp.pad(padded, ((0, 0), (1, 1), (1, 1), (0, 0)))

    def one_frame(position):
        slab = lax.dynamic_slice_in_dim(padded, position, 3, 0)
        summed = jnp.zeros((ROWS * COLS, COUT), jnp.float32)
        for a in range(3):
            for b in range(3):
                for c in range(3):
                    window = slab[a, b:b + ROWS, c:c + COLS, :].reshape(ROWS * COLS, CHANNELS)
                    summed = summed + jnp.dot(window, kernel[a, b, c], preferred_element_type=jnp.float32)
        return (summed.reshape(ROWS, COLS, COUT) + bias).astype(jnp.bfloat16)
    return lax.map(one_frame, jnp.arange(FRAMES, dtype=jnp.int32))
```

```python
import functools

import jax
import jax.numpy as jnp
from jax import lax
from jax.experimental import pallas as pl
from jax.experimental.pallas import tpu as pltpu
from jax.sharding import PartitionSpec as P

MESH = pl.DeviceIdType.MESH
GROUPS = 32
EPSILON = 1e-06


def offsets(count):
    every = [d if d <= count // 2 else d - count for d in range(1, count)]
    return sorted(every, key=lambda d: -abs(d))


def kernel(sizes, feat, gain, shift, weight, bias, out, raw, act, wbuf, obuf, gbuf, hbuf, bbuf,
           mine, row, got1, got2, in_sem, small_sem, w_sem, out_sem, s1, r1, s2, r2, hs, hr):
    tm_n, h_n = sizes
    y_n = tm_n // 2
    frames, rows, cols, channels = feat.shape
    lanes = 128
    parts = channels // lanes
    tm = lax.axis_index("tm")
    h = lax.axis_index("height")
    core = lax.rem(tm, 2)
    y = lax.div(tm, 2)
    first, last = tm == 0, tm == tm_n - 1
    top, bottom = h == 0, h == h_n - 1

    def turned(v, d, n):
        return lax.rem(v + (d + n), n)

    def near(dtm, dh):
        return {"tm": turned(tm, dtm, tm_n), "height": turned(h, dh, h_n)}

    def plane(dy, dc, dh):
        c = core if dc == 0 else 1 - core
        return {"tm": turned(y, dy, y_n) * 2 + c, "height": turned(h, dh, h_n)}

    peers1 = [(0, 1, dh) for dh in offsets(h_n)] + [(0, 0, dh) for dh in offsets(h_n)]
    peers1 = sorted(peers1 + [(0, 1, 0)], key=lambda p: -abs(p[2]))
    peers2 = [(dy, 0, 0) for dy in offsets(y_n)]
    halo = [(1, 0), (-1, 0), (1, 1), (-1, 1), (1, -1), (-1, -1)]

    own = pltpu.make_async_copy(feat, raw.at[frames:, 1 : 1 + rows], in_sem)
    own.start()
    smalls = [pltpu.make_async_copy(a, b, small_sem.at[i])
              for i, (a, b) in enumerate(((gain, gbuf), (shift, hbuf), (bias, bbuf)))]
    for copy in smalls:
        copy.start()
    weights = pltpu.make_async_copy(weight, wbuf, w_sem)
    weights.start()

    barrier = pltpu.get_barrier_semaphore()
    for p in peers1 + peers2:
        pl.semaphore_signal(barrier, inc=1, device_id=plane(*p), device_id_type=MESH)
    for p in halo:
        pl.semaphore_signal(barrier, inc=1, device_id=near(*p), device_id_type=MESH)

    own.wait()
    total = jnp.zeros((8, channels), jnp.float32)
    squares = jnp.zeros((8, channels), jnp.float32)
    for f in range(frames):
        for r in range(rows):
            x = raw[frames + f, 1 + r].astype(jnp.float32).reshape(cols // 8, 8, channels)
            total = total + jnp.sum(x, axis=0)
            squares = squares + jnp.sum(x * x, axis=0)
    total = jnp.sum(total, axis=0, keepdims=True)
    squares = jnp.sum(squares, axis=0, keepdims=True)
    for k in range(parts):
        mine[k : k + 1, :] = total[:, k * lanes : (k + 1) * lanes]
        mine[parts + k : parts + k + 1, :] = squares[:, k * lanes : (k + 1) * lanes]

    pl.semaphore_wait(barrier, len(peers1) + len(peers2) + len(halo))

    def send(src, dst, s, r, device):
        return pltpu.make_async_remote_copy(src_ref=src, dst_ref=dst, send_sem=s, recv_sem=r,
                                            device_id=device, device_id_type=MESH)

    for i, p in enumerate(peers1):
        send(mine, got1.at[i], s1, r1, plane(*p)).start()

    def edge(src_row, dst_row, frame, dtm, dh, i):
        return send(raw.at[frames:, src_row], raw.at[pl.ds(frame, frames), dst_row],
                    hs.at[i], hr.at[i], near(dtm, dh))

    down = edge(rows, 0, frames, 0, 1, 0)
    up = edge(1, rows + 1, frames, 0, -1, 1)
    down_next = edge(rows, 0, 0, 1, 1, 2)
    up_next = edge(1, rows + 1, 0, 1, -1, 3)
    along = send(raw.at[frames:, 1 : 1 + rows], raw.at[:frames, 1 : 1 + rows], hs.at[4], hr.at[4],
                 near(1, 0))
    sends = (
        (down, jnp.logical_not(bottom)),
        (up, jnp.logical_not(top)),
        (along, jnp.logical_not(last)),
        (down_next, jnp.logical_not(jnp.logical_or(bottom, last))),
        (up_next, jnp.logical_not(jnp.logical_or(top, last))),
    )
    arrivals = (
        (down, jnp.logical_not(top)),
        (up, jnp.logical_not(bottom)),
        (along, jnp.logical_not(first)),
        (down_next, jnp.logical_not(jnp.logical_or(top, first))),
        (up_next, jnp.logical_not(jnp.logical_or(bottom, first))),
    )
    for copy, there in sends:
        pl.when(there)(copy.start)

    everyone1 = send(got1, got1, s1, r1, near(1, 0))
    everyone1.wait_recv()
    here = mine[...]
    for i in range(len(peers1)):
        here = here + got1[i]
    row[...] = here
    for i, p in enumerate(peers2):
        send(row, got2.at[i], s2, r2, plane(*p)).start()

    for copy in smalls:
        copy.wait()
    weights.wait()
    for copy, there in arrivals:
        pl.when(there)(copy.wait_recv)

    everyone2 = send(got2, got2, s2, r2, near(1, 0))
    everyone2.wait_recv()
    for i in range(len(peers2)):
        here = here + got2[i]

    per_group = channels // GROUPS
    high = here.astype(jnp.bfloat16)
    rest = here - high.astype(jnp.float32)
    middle = rest.astype(jnp.bfloat16)
    low = (rest - middle.astype(jnp.float32)).astype(jnp.bfloat16)
    same = (lax.broadcasted_iota(jnp.int32, (lanes, lanes), 0) // per_group
            == lax.broadcasted_iota(jnp.int32, (lanes, lanes), 1) // per_group)
    same = jnp.where(same, 1.0, 0.0).astype(jnp.bfloat16)
    spread = sum(jnp.dot(a, same, preferred_element_type=jnp.float32) for a in (low, middle, high))
    cells = tm_n * h_n * frames * rows * cols * per_group
    spread = spread * (1.0 / cells)
    mean = spread[:parts]
    var = jnp.maximum(spread[parts:] - mean * mean, 0.0)
    scale = lax.rsqrt(var + EPSILON)

    def flat(a):
        return jnp.concatenate([a[k : k + 1] for k in range(parts)], axis=1)

    half_scale = flat(scale) * gbuf[...].reshape(1, channels) * 0.5
    half_shift = hbuf[...].reshape(1, channels) * 0.5 - flat(mean) * half_scale

    def activate(f, source, r):
        v = raw[source, r].astype(jnp.float32) * half_scale + half_shift
        act[f, r] = (v + v * jnp.tanh(v)).astype(jnp.bfloat16)

    for r in range(rows + 2):
        def line(r=r):
            for f in range(2 * frames):
                source = jnp.where(first, frames, f) if f < frames else f
                activate(f, source, r)

        def blank(r=r):
            for f in range(2 * frames):
                act[f, r] = jnp.zeros((cols, channels), jnp.bfloat16)

        if r == 0:
            pl.when(jnp.logical_not(top))(line)
            pl.when(top)(blank)
        elif r == rows + 1:
            pl.when(jnp.logical_not(bottom))(line)
            pl.when(bottom)(blank)
        else:
            line()

    offset = bbuf[...].reshape(1, 1, -1)
    m = rows * cols
    for f in range(frames):
        taps = []
        for c in range(3):
            acc = None
            for a in range(3):
                for b in range(3):
                    lhs = act[f + a, b : b + rows].reshape(m, channels)
                    part = jnp.dot(lhs, wbuf[a, b, c], preferred_element_type=jnp.float32)
                    acc = part if acc is None else acc + part
            taps.append(acc.reshape(rows, cols, -1))
        edge_zero = jnp.zeros((rows, 1, taps[0].shape[-1]), jnp.float32)
        left = jnp.concatenate([edge_zero, taps[0][:, :-1]], axis=1)
        right = jnp.concatenate([taps[2][:, 1:], edge_zero], axis=1)
        obuf[f] = (taps[1] + left + right + offset).astype(jnp.bfloat16)
    done = pltpu.make_async_copy(obuf, out, out_sem)
    done.start()
    done.wait()

    everyone1.wait_send()
    everyone2.wait_send()
    for copy, there in sends:
        pl.when(there)(copy.wait_send)


def solution(mesh):
    sizes = (mesh.shape["tm"], mesh.shape["height"])

    def on_device(features, gain, shift, weight, bias):
        frames, rows, cols, channels = features.shape
        cout = weight.shape[-1]
        n1 = 2 * sizes[1] - 1
        n2 = sizes[0] // 2 - 1
        any_space = pl.BlockSpec(memory_space=pl.ANY)
        slab = (2 * frames, rows + 2, cols, channels)
        dma = pltpu.SemaphoreType.DMA
        return pl.pallas_call(
            functools.partial(kernel, sizes),
            out_shape=jax.ShapeDtypeStruct((frames, rows, cols, cout), jnp.bfloat16),
            in_specs=[any_space] * 5,
            out_specs=any_space,
            scratch_shapes=[
                pltpu.VMEM(slab, jnp.bfloat16),
                pltpu.VMEM(slab, jnp.bfloat16),
                pltpu.VMEM(weight.shape, jnp.bfloat16),
                pltpu.VMEM((frames, rows, cols, cout), jnp.bfloat16),
                pltpu.VMEM((channels,), jnp.float32),
                pltpu.VMEM((channels,), jnp.float32),
                pltpu.VMEM((cout,), jnp.float32),
                pltpu.VMEM((8, 128), jnp.float32),
                pltpu.VMEM((8, 128), jnp.float32),
                pltpu.VMEM((n1, 8, 128), jnp.float32),
                pltpu.VMEM((n2, 8, 128), jnp.float32),
                dma, dma((3,)), dma, dma, dma, dma, dma, dma, dma((5,)), dma((5,)),
            ],
            compiler_params=pltpu.CompilerParams(
                collective_id=0, has_side_effects=True, vmem_limit_bytes=60 * 1024 * 1024
            ),
        )(features, gain, shift, weight, bias)

    return jax.shard_map(
        on_device,
        mesh=mesh,
        in_specs=(P(("clips", "tm"), "height", None, None), P(), P(), P(), P()),
        out_specs=P(("clips", "tm"), "height", None, None),
        check_vma=False,
    )
```

```python
import functools

import jax
import jax.numpy as jnp
from jax import lax
from jax.experimental import pallas as pl
from jax.experimental.pallas import tpu as pltpu
from jax.sharding import PartitionSpec as P

MESH = pl.DeviceIdType.MESH
GROUPS = 32
EPSILON = 1e-06


def kernel(sizes, feat, gain, shift, weight, bias, out, raw, act, wbuf, gbuf, hbuf, bbuf,
           mine, row, row2, late, span, got1, got2, in_sem, small_sem, w_sem, s0, r0, s1, r1, s2, r2, s4, hs, hr, perm0, perm2, perm3):
    tm_n, h_n = sizes
    y_n = tm_n // 2
    frames, rows, cols, channels = feat.shape
    lanes = 128
    parts = channels // lanes
    tm = lax.axis_index("tm")
    h = lax.axis_index("height")
    core = lax.rem(tm, 2)
    y = lax.div(tm, 2)
    first, last = tm == 0, tm == tm_n - 1
    top, bottom = h == 0, h == h_n - 1

    wide = 2 * h_n
    rank = core * h_n + h
    leader = jnp.logical_and(first, top)
    member = jnp.logical_not(leader)
    all_of, any_of, no = jnp.logical_and, jnp.logical_or, jnp.logical_not
    passes_on = any_of(all_of(core == 0, member), all_of(tm == 1, top))
    receives_along = all_of(core == 0, no(first))

    def at(dtm, dh):
        return {"tm": tm + dtm, "height": h + dh}

    def chip_row(q, frame_chip=y):
        return {"tm": frame_chip * 2 + q // h_n, "height": q % h_n}

    def column(other, c):
        return {"tm": other * 2 + c, "height": h}

    far = sorted(range(wide), key=lambda q: (-min(q % h_n, h_n - q % h_n), q))

    def when(condition, f, *args):
        pl.when(condition)(functools.partial(f, *args))

    def signal(sem, device):
        pl.semaphore_signal(sem, inc=1, device_id=device, device_id_type=MESH)

    def send(src, dst, s, r, device):
        return pltpu.make_async_remote_copy(src_ref=src, dst_ref=dst, send_sem=s, recv_sem=r,
                                            device_id=device, device_id_type=MESH)

    loads = {}
    for f in range(frames):
        for r in range(rows):
            loads[f, r] = pltpu.make_async_copy(feat.at[f, r], raw.at[frames + f, 1 + r], in_sem.at[f, r])
            loads[f, r].start()
    smalls = [pltpu.make_async_copy(a, b, small_sem.at[i])
              for i, (a, b) in enumerate(((gain, gbuf), (shift, hbuf), (bias, bbuf)))]
    for copy in smalls:
        copy.start()
    weights = pltpu.make_async_copy(weight, wbuf, w_sem)
    weights.start()

    barrier = pltpu.get_barrier_semaphore()

    @pl.when(member)
    def _():
        when(any_of(y == 0, rank == 0), signal, barrier, {"tm": 0, "height": 0})
        for q in range(wide):
            ahead = q != rank if q else all_of(rank > 0, y > 0)
            when(ahead, signal, barrier, chip_row(q))
        for other in range(1, y_n):
            when(other > y, signal, barrier, column(other, 0))
            when(other > y, signal, barrier, column(other, 1))
        when(receives_along, signal, barrier, at(-1, 0))
        when(all_of(receives_along, no(top)), signal, barrier, at(-1, -1))
        when(all_of(receives_along, no(bottom)), signal, barrier, at(-1, 1))

    total = jnp.zeros((8, channels), jnp.float32)
    squares = jnp.zeros((8, channels), jnp.float32)
    for f, r in loads:
        loads[f, r].wait()
        x = raw[frames + f, 1 + r].astype(jnp.float32).reshape(cols // 8, 8, channels)
        total = total + jnp.sum(x, axis=0)
        squares = squares + jnp.sum(x * x, axis=0)
    total = jnp.sum(total, axis=0, keepdims=True)
    squares = jnp.sum(squares, axis=0, keepdims=True)
    for k in range(parts):
        mine[k : k + 1, :] = total[:, k * lanes : (k + 1) * lanes]
        mine[parts + k : parts + k + 1, :] = squares[:, k * lanes : (k + 1) * lanes]

    def number(condition):
        return condition.astype(jnp.int32)

    beside = wide - 1 - number(y == 0)
    below = 2 * y - number(all_of(top, y > 0))
    onward = number(all_of(core == 1, no(last))) * (3 - number(top) - number(bottom))
    everybody = wide - 1 + y_n - 1
    pl.semaphore_wait(barrier, jnp.where(leader, everybody, beside + below + onward))

    def edge(src_row, dst_row, frame, dtm, dh, i):
        return send(raw.at[frames:, src_row], raw.at[pl.ds(frame, frames), dst_row],
                    hs.at[i], hr.at[i], at(dtm, dh))

    down = edge(rows, 0, frames, 0, 1, 0)
    up = edge(1, rows + 1, frames, 0, -1, 1)
    down_next = edge(rows, 0, 0, 1, 1, 2)
    up_next = edge(1, rows + 1, 0, 1, -1, 3)
    along = send(raw.at[frames:, 1 : 1 + rows], raw.at[:frames, 1 : 1 + rows], hs.at[4], hr.at[4],
                 at(1, 0))
    down_again = edge(0, 0, 0, 1, 0, 2)
    up_again = edge(rows + 1, rows + 1, 0, 1, 0, 3)
    to_leader = all_of(first, h == 1)
    sends = (
        (down, no(bottom)),
        (along, no(last)),
        (down_next, all_of(core == 1, no(any_of(bottom, last)))),
        (up_next, any_of(to_leader, all_of(core == 1, no(any_of(top, last))))),
        (up, all_of(no(top), no(to_leader))),
    )
    arrivals = (
        (down, no(top)),
        (up, no(bottom)),
        (along, no(first)),
        (down_next, no(any_of(top, first))),
        (up_next, no(any_of(bottom, first))),
    )

    def tell(device):
        return send(mine, late, s0, r0, device)

    @pl.when(leader)
    def _():
        for q in far:
            if q:
                tell(chip_row(q, 0)).start()
        signal(perm0, {"tm": 0, "height": 1})
        signal(perm0, {"tm": 1, "height": 0})

    def give(q):
        send(mine, got1.at[rank], s1.at[q], r1.at[rank], chip_row(q)).start()

    @pl.when(member)
    def _():
        for other in range(y_n - 1):
            sender = jnp.where(top, 1, 0) if other == 0 else 0
            when(other < y, signal, perm2.at[y], column(other, sender))
        when(all_of(y > 0, rank > 0), signal, perm3, column(0, core))
        for q in far:
            ahead = q != rank if q else all_of(rank > 0, y > 0)
            when(ahead, give, q)

    for copy, there in sends:
        when(there, copy.start)

    @pl.when(leader)
    def _():
        for other in range(1, y_n):
            tell(column(other, 0)).start()

    @pl.when(member)
    def _():
        got1[rank] = mine[...]

        @pl.when(y == 0)
        def _():
            got1[0] = jnp.zeros_like(mine)

        for q in range(wide):
            ahead = q != rank if q else all_of(rank > 0, y > 0)
            when(ahead, send(mine, got1.at[q], s1.at[q], r1.at[q], chip_row(q)).wait)
        here = got1[0]
        for q in range(1, wide):
            here = here + got1[q]
        row[...] = here
        got2[y] = here

        def pass_on(other, c):
            send(row, got2.at[y], s2.at[other, c], r2.at[y], column(other, c)).start()

        @pl.when(passes_on)
        def _():
            for other in range(y_n):
                @pl.when(other != y)
                def _():
                    when(other > y, pl.semaphore_wait, perm2.at[other], 2)
                    if other:
                        pass_on(other, 0)
                    else:
                        when(no(top), pass_on, other, 0)
                    pass_on(other, 1)

        @pl.when(to_leader)
        def _():
            pl.semaphore_wait(perm0, 1)
            up.start()

        for other in range(y_n):
            when(other != y, send(row, got2.at[other], s2.at[0, 0], r2.at[other], column(other, 0)).wait_recv)
        here = got2[0]
        for other in range(1, y_n):
            here = here + got2[other]
        row2[...] = here

        @pl.when(all_of(tm == 1, top))
        def _():
            pl.semaphore_wait(perm0, 1)
            send(row2, late, s0, r0, {"tm": 0, "height": 0}).start()

    @pl.when(leader)
    def _():
        row2[...] = mine[...]

    relays = all_of(member, y == 0)
    tell(at(0, 0)).wait_recv()

    @pl.when(relays)
    def _():
        pl.semaphore_wait(perm3, y_n - 1)
        for other in range(1, y_n):
            send(late, late, s4.at[other], r0, column(other, core)).start()

    for copy in smalls:
        copy.wait()
    weights.wait()
    when(no(top), down.wait_recv)
    when(all_of(core == 0, no(top)), down_again.start)
    when(no(bottom), up.wait_recv)
    when(all_of(all_of(core == 0, no(bottom)), member), up_again.start)
    for copy, there in arrivals[2:]:
        when(there, copy.wait_recv)
    here = row2[...] + late[...]

    per_group = channels // GROUPS
    high = here.astype(jnp.bfloat16)
    rest = here - high.astype(jnp.float32)
    middle = rest.astype(jnp.bfloat16)
    low = (rest - middle.astype(jnp.float32)).astype(jnp.bfloat16)
    same = (lax.broadcasted_iota(jnp.int32, (lanes, lanes), 0) // per_group
            == lax.broadcasted_iota(jnp.int32, (lanes, lanes), 1) // per_group)
    same = jnp.where(same, 1.0, 0.0).astype(jnp.bfloat16)
    spread = sum(jnp.dot(a, same, preferred_element_type=jnp.float32) for a in (low, middle, high))
    cells = tm_n * h_n * frames * rows * cols * per_group
    spread = spread * (1.0 / cells)
    mean = spread[:parts]
    var = jnp.maximum(spread[parts:] - mean * mean, 0.0)
    scale = lax.rsqrt(var + EPSILON)

    def flat(a):
        return jnp.concatenate([a[k : k + 1] for k in range(parts)], axis=1)

    half_scale = flat(scale) * gbuf[...].reshape(1, channels) * 0.5
    half_shift = hbuf[...].reshape(1, channels) * 0.5 - flat(mean) * half_scale

    def activate(f, source, r):
        v = raw[source, r].astype(jnp.float32) * half_scale + half_shift
        act[f, r] = (v + v * jnp.tanh(v)).astype(jnp.bfloat16)

    for r in range(rows + 2):
        def line(r=r):
            for f in range(2 * frames):
                source = jnp.where(first, frames, f) if f < frames else f
                activate(f, source, r)

        def blank(r=r):
            for f in range(2 * frames):
                act[f, r] = jnp.zeros((cols, channels), jnp.bfloat16)

        if r == 0:
            pl.when(jnp.logical_not(top))(line)
            pl.when(top)(blank)
        elif r == rows + 1:
            pl.when(jnp.logical_not(bottom))(line)
            pl.when(bottom)(blank)
        else:
            line()

    offset = bbuf[...].reshape(1, 1, -1)
    m = rows * cols
    for f in range(frames):
        taps = []
        for c in range(3):
            acc = None
            for a in range(3):
                for b in range(3):
                    lhs = act[f + a, b : b + rows].reshape(m, channels)
                    part = jnp.dot(lhs, wbuf[a, b, c], preferred_element_type=jnp.float32)
                    acc = part if acc is None else acc + part
            taps.append(acc.reshape(rows, cols, -1))
        edge_zero = jnp.zeros((rows, 1, taps[0].shape[-1]), jnp.float32)
        left = jnp.concatenate([edge_zero, taps[0][:, :-1]], axis=1)
        right = jnp.concatenate([taps[2][:, 1:], edge_zero], axis=1)
        out[f] = (taps[1] + left + right + offset).astype(jnp.bfloat16)
    @pl.when(leader)
    def _():
        send(span, span, s0, r0, at(0, 0)).wait_send()

    @pl.when(relays)
    def _():
        for other in range(1, y_n):
            send(late, late, s4.at[other], r0, at(0, 0)).wait_send()

    when(all_of(tm == 1, top), send(row2, late, s0, r0, at(0, 0)).wait_send)

    @pl.when(passes_on)
    def _():
        for other in range(y_n):
            for c in range(2):
                sent = other != y if other or c else all_of(other != y, no(top))
                when(sent, send(row, row, s2.at[other, c], r2.at[0], at(0, 0)).wait_send)

    for copy, there in sends[:-1]:
        when(there, copy.wait_send)
    when(no(top), up.wait_send)
    when(all_of(core == 0, no(top)), down_again.wait_send)
    when(all_of(all_of(core == 0, no(bottom)), member), up_again.wait_send)


def solution(mesh):
    sizes = (mesh.shape["tm"], mesh.shape["height"])

    def on_device(features, gain, shift, weight, bias):
        frames, rows, cols, channels = features.shape
        cout = weight.shape[-1]
        n1 = 2 * sizes[1]
        n2 = sizes[0] // 2
        any_space = pl.BlockSpec(memory_space=pl.ANY)
        slab = (2 * frames, rows + 2, cols, channels)
        dma = pltpu.SemaphoreType.DMA
        return pl.pallas_call(
            functools.partial(kernel, sizes),
            out_shape=pltpu.VMEM((frames, rows, cols, cout), jnp.bfloat16),
            in_specs=[any_space] * 5,
            out_specs=pl.BlockSpec(memory_space=pltpu.VMEM),
            scratch_shapes=[
                pltpu.VMEM(slab, jnp.bfloat16),
                pltpu.VMEM(slab, jnp.bfloat16),
                pltpu.VMEM(weight.shape, jnp.bfloat16),
                pltpu.VMEM((channels,), jnp.float32),
                pltpu.VMEM((channels,), jnp.float32),
                pltpu.VMEM((cout,), jnp.float32),
                pltpu.VMEM((8, 128), jnp.float32),
                pltpu.VMEM((8, 128), jnp.float32),
                pltpu.VMEM((8, 128), jnp.float32),
                pltpu.VMEM((8, 128), jnp.float32),
                pltpu.VMEM((n1 + n2 - 2, 8, 128), jnp.float32),
                pltpu.VMEM((n1, 8, 128), jnp.float32),
                pltpu.VMEM((n2, 8, 128), jnp.float32),
                dma((frames, rows)), dma((3,)), dma, dma, dma, dma((n1,)), dma((n1,)), dma((n2, 2)), dma((n2,)),
                dma((n2,)), dma((5,)), dma((5,)), pltpu.SemaphoreType.REGULAR, pltpu.SemaphoreType.REGULAR((n2,)),
                pltpu.SemaphoreType.REGULAR,
            ],
            compiler_params=pltpu.CompilerParams(
                collective_id=0, has_side_effects=True, vmem_limit_bytes=60 * 1024 * 1024
            ),
        )(features, gain, shift, weight, bias)

    return jax.shard_map(
        on_device,
        mesh=mesh,
        in_specs=(P(("clips", "tm"), "height", None, None), P(), P(), P(), P()),
        out_specs=P(("clips", "tm"), "height", None, None),
        check_vma=False,
    )
```

```python
import functools

import jax
import jax.numpy as jnp
from jax import lax
from jax.experimental import pallas as pl
from jax.experimental.pallas import tpu as pltpu
from jax.sharding import PartitionSpec as P

MESH = pl.DeviceIdType.MESH
GROUPS = 32
EPSILON = 1e-06


def kernel(sizes, feat, gain, shift, weight, bias, out, raw, act, wbuf, mixed, sums, gbuf, hbuf, bbuf,
           mine, row, row2, late, span, got1, got2, in_sem, small_sem, w_sem, s0, r0, s1, r1, s2, r2, s4, hs, hr, perm0, perm2, perm3):
    tm_n, h_n = sizes
    y_n = tm_n // 2
    frames, rows, cols, channels = feat.shape
    lanes = 128
    parts = channels // lanes
    tm = lax.axis_index("tm")
    h = lax.axis_index("height")
    core = lax.rem(tm, 2)
    y = lax.div(tm, 2)
    first, last = tm == 0, tm == tm_n - 1
    top, bottom = h == 0, h == h_n - 1

    wide = 2 * h_n
    rank = core * h_n + h
    leader = jnp.logical_and(first, top)
    member = jnp.logical_not(leader)
    all_of, any_of, no = jnp.logical_and, jnp.logical_or, jnp.logical_not
    passes_on = any_of(all_of(core == 0, member), all_of(tm == 1, top))
    receives_along = all_of(core == 0, no(first))

    def at(dtm, dh):
        return {"tm": tm + dtm, "height": h + dh}

    def chip_row(q, frame_chip=y):
        return {"tm": frame_chip * 2 + q // h_n, "height": q % h_n}

    def column(other, c):
        return {"tm": other * 2 + c, "height": h}

    far = sorted(range(wide), key=lambda q: (-min(q % h_n, h_n - q % h_n), q))

    def when(condition, f, *args):
        pl.when(condition)(functools.partial(f, *args))

    def signal(sem, device):
        pl.semaphore_signal(sem, inc=1, device_id=device, device_id_type=MESH)

    def send(src, dst, s, r, device):
        return pltpu.make_async_remote_copy(src_ref=src, dst_ref=dst, send_sem=s, recv_sem=r,
                                            device_id=device, device_id_type=MESH)

    loads = {}
    for f in range(frames):
        for r in range(rows):
            loads[f, r] = pltpu.make_async_copy(feat.at[f, r], raw.at[frames + f, 1 + r], in_sem.at[f, r])
            loads[f, r].start()
    smalls = [pltpu.make_async_copy(a, b, small_sem.at[i])
              for i, (a, b) in enumerate(((gain, gbuf), (shift, hbuf), (bias, bbuf)))]
    for copy in smalls:
        copy.start()
    weights = pltpu.make_async_copy(weight, wbuf, w_sem)
    weights.start()

    barrier = pltpu.get_barrier_semaphore()

    @pl.when(member)
    def _():
        when(any_of(y == 0, rank == 0), signal, barrier, {"tm": 0, "height": 0})
        for q in range(wide):
            ahead = q != rank if q else all_of(rank > 0, y > 0)
            when(ahead, signal, barrier, chip_row(q))
        for other in range(1, y_n):
            when(other > y, signal, barrier, column(other, 0))
            when(other > y, signal, barrier, column(other, 1))
        when(receives_along, signal, barrier, at(-1, 0))
        when(all_of(receives_along, no(top)), signal, barrier, at(-1, -1))
        when(all_of(receives_along, no(bottom)), signal, barrier, at(-1, 1))

    total = jnp.zeros((8, channels), jnp.float32)
    squares = jnp.zeros((8, channels), jnp.float32)
    for f, r in loads:
        loads[f, r].wait()
        x = raw[frames + f, 1 + r].astype(jnp.float32).reshape(cols // 8, 8, channels)
        total = total + jnp.sum(x, axis=0)
        squares = squares + jnp.sum(x * x, axis=0)
    total = jnp.sum(total, axis=0, keepdims=True)
    squares = jnp.sum(squares, axis=0, keepdims=True)
    for k in range(parts):
        mine[k : k + 1, :] = total[:, k * lanes : (k + 1) * lanes]
        mine[parts + k : parts + k + 1, :] = squares[:, k * lanes : (k + 1) * lanes]

    def number(condition):
        return condition.astype(jnp.int32)

    beside = wide - 1 - number(y == 0)
    below = 2 * y - number(all_of(top, y > 0))
    onward = number(all_of(core == 1, no(last))) * (3 - number(top) - number(bottom))
    everybody = wide - 1 + y_n - 1
    pl.semaphore_wait(barrier, jnp.where(leader, everybody, beside + below + onward))

    def edge(src_row, dst_row, frame, dtm, dh, i):
        return send(raw.at[frames:, src_row], raw.at[pl.ds(frame, frames), dst_row],
                    hs.at[i], hr.at[i], at(dtm, dh))

    down = edge(rows, 0, frames, 0, 1, 0)
    up = edge(1, rows + 1, frames, 0, -1, 1)
    down_next = edge(rows, 0, 0, 1, 1, 2)
    up_next = edge(1, rows + 1, 0, 1, -1, 3)
    along = send(raw.at[frames:, 1 : 1 + rows], raw.at[:frames, 1 : 1 + rows], hs.at[4], hr.at[4],
                 at(1, 0))
    down_again = edge(0, 0, 0, 1, 0, 2)
    up_again = edge(rows + 1, rows + 1, 0, 1, 0, 3)
    to_leader = all_of(first, h == 1)
    sends = (
        (down, no(bottom)),
        (along, no(last)),
        (down_next, all_of(core == 1, no(any_of(bottom, last)))),
        (up_next, any_of(to_leader, all_of(core == 1, no(any_of(top, last))))),
        (up, all_of(no(top), no(to_leader))),
    )
    along_ends = no(first)
    arrivals = (
        (down, no(top)),
        (up, no(bottom)),
        (along, no(first)),
        (down_next, no(any_of(top, first))),
        (up_next, no(any_of(bottom, first))),
    )

    def tell(device):
        return send(mine, late, s0, r0, device)

    @pl.when(leader)
    def _():
        for q in far:
            if q:
                tell(chip_row(q, 0)).start()
        signal(perm0, {"tm": 0, "height": 1})
        signal(perm0, {"tm": 1, "height": 0})

    def hand_on():
        when(no(top), down.wait_recv)
        when(all_of(core == 0, no(top)), down_again.start)
        when(no(bottom), up.wait_recv)
        when(all_of(all_of(core == 0, no(bottom)), member), up_again.start)

    def give(q):
        send(mine, got1.at[rank], s1.at[q], r1.at[rank], chip_row(q)).start()

    @pl.when(member)
    def _():
        for other in range(y_n - 1):
            sender = jnp.where(top, 1, 0) if other == 0 else 0
            when(other < y, signal, perm2.at[y], column(other, sender))
        when(all_of(y > 0, rank > 0), signal, perm3, column(0, core))
        for q in far:
            ahead = q != rank if q else all_of(rank > 0, y > 0)
            when(ahead, give, q)

    for copy, there in sends:
        when(there, copy.start)

    @pl.when(leader)
    def _():
        for other in range(1, y_n):
            tell(column(other, 0)).start()

    @pl.when(member)
    def _():
        got1[rank] = mine[...]

        @pl.when(y == 0)
        def _():
            got1[0] = jnp.zeros_like(mine)

        for q in range(wide):
            ahead = q != rank if q else all_of(rank > 0, y > 0)
            when(ahead, send(mine, got1.at[q], s1.at[q], r1.at[q], chip_row(q)).wait)
        here = got1[0]
        for q in range(1, wide):
            here = here + got1[q]
        row[...] = here
        got2[y] = here

        def pass_on(other, c):
            send(row, got2.at[y], s2.at[other, c], r2.at[y], column(other, c)).start()

        @pl.when(passes_on)
        def _():
            for other in range(y_n):
                @pl.when(other != y)
                def _():
                    when(other > y, pl.semaphore_wait, perm2.at[other], 2)
                    if other:
                        pass_on(other, 0)
                    else:
                        when(no(top), pass_on, other, 0)
                    pass_on(other, 1)

    weights.wait()

    @pl.loop(0, 9)
    def _(i):
        a, c = i // 3, lax.rem(i, 3)
        for k in range(0, channels, 64):
            g0, g1, g2 = (wbuf[a, b, c, k : k + 64].astype(jnp.float32) for b in range(3))
            even, odd = 0.5 * (g0 + g2), 0.5 * g1
            mixed[a, 0, c, k : k + 64] = (even + odd).astype(jnp.bfloat16)
            mixed[a, 1, c, k : k + 64] = (even - odd).astype(jnp.bfloat16)

    @pl.when(member)
    def _():
        @pl.when(to_leader)
        def _():
            pl.semaphore_wait(perm0, 1)
            up.start()

        when(no(to_leader), hand_on)

        for other in range(y_n):
            when(other != y, send(row, got2.at[other], s2.at[0, 0], r2.at[other], column(other, 0)).wait_recv)
        here = got2[0]
        for other in range(1, y_n):
            here = here + got2[other]
        row2[...] = here

        @pl.when(all_of(tm == 1, top))
        def _():
            pl.semaphore_wait(perm0, 1)
            send(row2, late, s0, r0, {"tm": 0, "height": 0}).start()

    @pl.when(leader)
    def _():
        row2[...] = mine[...]

    relays = all_of(member, y == 0)
    tell(at(0, 0)).wait_recv()

    @pl.when(relays)
    def _():
        pl.semaphore_wait(perm3, y_n - 1)
        for other in range(1, y_n):
            send(late, late, s4.at[other], r0, column(other, core)).start()

    for copy in smalls:
        copy.wait()
    when(along_ends, along.wait_recv)
    here = row2[...] + late[...]

    per_group = channels // GROUPS
    high = here.astype(jnp.bfloat16)
    rest = here - high.astype(jnp.float32)
    middle = rest.astype(jnp.bfloat16)
    low = (rest - middle.astype(jnp.float32)).astype(jnp.bfloat16)
    same = (lax.broadcasted_iota(jnp.int32, (lanes, lanes), 0) // per_group
            == lax.broadcasted_iota(jnp.int32, (lanes, lanes), 1) // per_group)
    same = jnp.where(same, 1.0, 0.0).astype(jnp.bfloat16)
    spread = sum(jnp.dot(a, same, preferred_element_type=jnp.float32) for a in (low, middle, high))
    cells = tm_n * h_n * frames * rows * cols * per_group
    spread = spread * (1.0 / cells)
    mean = spread[:parts]
    var = jnp.maximum(spread[parts:] - mean * mean, 0.0)
    scale = lax.rsqrt(var + EPSILON)

    def flat(a):
        return jnp.concatenate([a[k : k + 1] for k in range(parts)], axis=1)

    half_scale = flat(scale) * gbuf[...].reshape(1, channels) * 0.5
    half_shift = hbuf[...].reshape(1, channels) * 0.5 - flat(mean) * half_scale

    step = 16

    def activated(f, r, k):
        source = jnp.where(first, frames, f) if f < frames else f
        v = raw[source, r, k : k + step].astype(jnp.float32) * half_scale + half_shift
        return v + v * jnp.tanh(v)

    def put(p, f, pair, k, value):
        act[p, f, pair, k : k + step] = value.astype(jnp.bfloat16)

    for f in range(2 * frames):
        for k in range(0, cols, step):
            d = [activated(f, r, k) for r in range(1, rows + 1)]
            for pair in range(2):
                put(1, f, pair, k, d[2 * pair] + d[2 * pair + 1])
                put(2, f, pair, k, d[2 * pair + 1] - d[2 * pair])
            put(0, f, 1, k, d[1] - d[3])
            put(3, f, 0, k, d[0] - d[2])

    m = frames * 2 * cols

    def product(p, c):
        acc = None
        for a in range(3):
            lhs = act[p, a : a + frames].reshape(m, channels)
            rhs = wbuf[a, 2 * (p // 3), c] if p in (0, 3) else mixed[a, p - 1, c]
            part = jnp.dot(lhs, rhs, preferred_element_type=jnp.float32)
            acc = part if acc is None else acc + part
        return acc

    for c in range(3):
        m1, m2 = product(1, c), product(2, c)
        sums[c, 0] = m1 + m2
        sums[c, 1] = m1 - m2

    @pl.when(no(leader))
    def _():
        when(to_leader, hand_on)
        for copy, there in arrivals[3:]:
            when(there, copy.wait_recv)

    when(leader, hand_on)

    for f in range(2 * frames):
        for k in range(0, cols, step):
            above = jnp.where(top, 0.0, activated(f, 0, k))
            below = jnp.where(bottom, 0.0, activated(f, rows + 1, k))
            put(0, f, 0, k, above - activated(f, 2, k))
            put(3, f, 1, k, activated(f, rows - 1, k) - below)

    offset = bbuf[...].reshape(1, -1)
    for c in range(3):
        sums[c, 0] = sums[c, 0] + product(0, c)
        sums[c, 1] = sums[c, 1] - product(3, c)
    for odd in range(2):
        for f in range(frames):
            for pair in range(2):
                at0 = (f * 2 + pair) * cols
                left, middle, right = (sums[c, odd, at0 : at0 + cols] for c in range(3))
                zero = jnp.zeros_like(left[:1])
                left = jnp.concatenate([zero, left[:-1]], axis=0)
                right = jnp.concatenate([right[1:], zero], axis=0)
                out[f, 2 * pair + odd] = (middle + left + right + offset).astype(jnp.bfloat16)

    @pl.when(leader)
    def _():
        send(span, span, s0, r0, at(0, 0)).wait_send()

    @pl.when(relays)
    def _():
        for other in range(1, y_n):
            send(late, late, s4.at[other], r0, at(0, 0)).wait_send()

    when(all_of(tm == 1, top), send(row2, late, s0, r0, at(0, 0)).wait_send)

    @pl.when(passes_on)
    def _():
        for other in range(y_n):
            for c in range(2):
                sent = other != y if other or c else all_of(other != y, no(top))
                when(sent, send(row, row, s2.at[other, c], r2.at[0], at(0, 0)).wait_send)

    for copy, there in sends[:-1]:
        when(there, copy.wait_send)
    when(no(top), up.wait_send)
    when(all_of(core == 0, no(top)), down_again.wait_send)
    when(all_of(all_of(core == 0, no(bottom)), member), up_again.wait_send)


def solution(mesh):
    sizes = (mesh.shape["tm"], mesh.shape["height"])

    def on_device(features, gain, shift, weight, bias):
        frames, rows, cols, channels = features.shape
        cout = weight.shape[-1]
        n1 = 2 * sizes[1]
        n2 = sizes[0] // 2
        any_space = pl.BlockSpec(memory_space=pl.ANY)
        slab = (2 * frames, rows + 2, cols, channels)
        dma = pltpu.SemaphoreType.DMA
        return pl.pallas_call(
            functools.partial(kernel, sizes),
            out_shape=pltpu.VMEM((frames, rows, cols, cout), jnp.bfloat16),
            in_specs=[any_space] * 5,
            out_specs=pl.BlockSpec(memory_space=pltpu.VMEM),
            scratch_shapes=[
                pltpu.VMEM(slab, jnp.bfloat16),
                pltpu.VMEM((4, 2 * frames, 2, cols, channels), jnp.bfloat16),
                pltpu.VMEM(weight.shape, jnp.bfloat16),
                pltpu.VMEM((3, 2, 3, channels, cout), jnp.bfloat16),
                pltpu.VMEM((3, 2, frames * 2 * cols, cout), jnp.float32),
                pltpu.VMEM((channels,), jnp.float32),
                pltpu.VMEM((channels,), jnp.float32),
                pltpu.VMEM((cout,), jnp.float32),
                pltpu.VMEM((8, 128), jnp.float32),
                pltpu.VMEM((8, 128), jnp.float32),
                pltpu.VMEM((8, 128), jnp.float32),
                pltpu.VMEM((8, 128), jnp.float32),
                pltpu.VMEM((n1 + n2 - 2, 8, 128), jnp.float32),
                pltpu.VMEM((n1, 8, 128), jnp.float32),
                pltpu.VMEM((n2, 8, 128), jnp.float32),
                dma((frames, rows)), dma((3,)), dma, dma, dma, dma((n1,)), dma((n1,)), dma((n2, 2)), dma((n2,)),
                dma((n2,)), dma((5,)), dma((5,)), pltpu.SemaphoreType.REGULAR, pltpu.SemaphoreType.REGULAR((n2,)),
                pltpu.SemaphoreType.REGULAR,
            ],
            compiler_params=pltpu.CompilerParams(
                collective_id=0, has_side_effects=True, vmem_limit_bytes=60 * 1024 * 1024
            ),
        )(features, gain, shift, weight, bias)

    return jax.shard_map(
        on_device,
        mesh=mesh,
        in_specs=(P(("clips", "tm"), "height", None, None), P(), P(), P(), P()),
        out_specs=P(("clips", "tm"), "height", None, None),
        check_vma=False,
    )
```

```python
import functools

import jax
import jax.numpy as jnp
from jax import lax
from jax.experimental import pallas as pl
from jax.experimental.pallas import tpu as pltpu
from jax.sharding import PartitionSpec as P

MESH = pl.DeviceIdType.MESH
GROUPS = 32
EPSILON = 1e-06


def kernel(sizes, feat, gain, shift, weight, bias, out, raw, act, wbuf, mixed, sums, kept, gbuf, hbuf, bbuf,
           mine, pair, row, row2, late, span, got1, got2, in_sem, small_sem, w_sem, s0, r0, s1, r1, s2, r2, s4, s5, hs, hr, perm0, perm2):
    tm_n, h_n = sizes
    y_n = tm_n // 2
    frames, rows, cols, channels = feat.shape
    lanes = 128
    parts = channels // lanes
    tm = lax.axis_index("tm")
    h = lax.axis_index("height")
    core = lax.rem(tm, 2)
    y = lax.div(tm, 2)
    first, last = tm == 0, tm == tm_n - 1
    top, bottom = h == 0, h == h_n - 1

    wide = 2 * h_n
    leader = jnp.logical_and(first, top)
    member = jnp.logical_not(leader)
    all_of, any_of, no = jnp.logical_and, jnp.logical_or, jnp.logical_not
    beside_leader = all_of(tm == 1, top)
    passes_on = any_of(all_of(core == 0, member), beside_leader)
    receives_along = all_of(core == 0, no(first))
    to_leader = all_of(first, h == 1)

    def at(dtm, dh):
        return {"tm": tm + dtm, "height": h + dh}

    def in_row(other, c, chip=y):
        return {"tm": chip * 2 + c, "height": other}

    def column(other, c):
        return {"tm": other * 2 + c, "height": h}

    def turn(v):
        half = h_n // 2
        if isinstance(v, int):
            return v if v < half else half + h_n - 1 - v
        return jnp.where(v < half, v, half + h_n - 1 - v)

    here_turn = turn(h)
    def when(condition, f, *args):
        pl.when(condition)(functools.partial(f, *args))

    def signal(sem, device):
        pl.semaphore_signal(sem, inc=1, device_id=device, device_id_type=MESH)

    def send(src, dst, s, r, device):
        return pltpu.make_async_remote_copy(src_ref=src, dst_ref=dst, send_sem=s, recv_sem=r,
                                            device_id=device, device_id_type=MESH)

    loads = {}
    for f in range(frames):
        for r in range(rows):
            loads[f, r] = pltpu.make_async_copy(feat.at[f, r], raw.at[frames + f, 1 + r], in_sem.at[f, r])
            loads[f, r].start()
    smalls = [pltpu.make_async_copy(a, b, small_sem.at[i])
              for i, (a, b) in enumerate(((gain, gbuf), (shift, hbuf), (bias, bbuf)))]
    for copy in smalls:
        copy.start()
    weights = pltpu.make_async_copy(weight, wbuf, w_sem)
    weights.start()

    barrier = pltpu.get_barrier_semaphore()

    @pl.when(member)
    def _():
        for other in range(1, h_n):
            @pl.when(turn(other) > here_turn)
            def _():
                signal(barrier, in_row(other, 0))
                signal(barrier, in_row(other, 1))
        when(no(beside_leader), signal, barrier, column(y, 1 - core))
        when(no(top), signal, barrier, at(0, -1))
        when(no(bottom), signal, barrier, at(0, 1))

        @pl.when(receives_along)
        def _():
            signal(barrier, at(-1, 0))
            when(no(top), signal, barrier, at(-1, -1))
            when(no(bottom), signal, barrier, at(-1, 1))

        when(any_of(y == 0, all_of(core == 0, top)), signal, barrier, {"tm": 0, "height": 0})
        for other in range(1, y_n):
            @pl.when(other > y)
            def _():
                signal(barrier, column(other, 0))
                signal(barrier, column(other, 1))

    def number(condition):
        return condition.astype(jnp.int32)

    above_it = 2 * y - number(all_of(top, y > 0)) + 1 - number(beside_leader)
    before_it = 2 * here_turn - number(all_of(y == 0, h > 0))
    edges = number(no(bottom)) + number(no(top)) - number(to_leader)
    onward = number(all_of(core == 1, no(last))) * (3 - number(top) - number(bottom))
    for_leader = (wide - 1) + (y_n - 1) + 1
    def edge(src_row, dst_row, frame, dtm, dh, i):
        return send(raw.at[frames:, src_row], raw.at[pl.ds(frame, frames), dst_row],
                    hs.at[i], hr.at[i], at(dtm, dh))

    down = edge(rows, 0, frames, 0, 1, 0)
    up = edge(1, rows + 1, frames, 0, -1, 1)
    down_next = edge(rows, 0, 0, 1, 1, 2)
    up_next = edge(1, rows + 1, 0, 1, -1, 3)
    along = send(raw.at[frames:, 1 : 1 + rows], raw.at[:frames, 1 : 1 + rows], hs.at[4], hr.at[4],
                 at(1, 0))
    down_again = edge(0, 0, 0, 1, 0, 2)
    up_again = edge(rows + 1, rows + 1, 0, 1, 0, 3)
    down_beside = send(raw.at[:frames, rows], raw.at[:frames, 0], s5, hr.at[2], at(0, 1))
    for load in loads.values():
        load.wait()

    @pl.when(leader)
    def _():
        pl.semaphore_wait(barrier, for_leader)
        along.start()

    total = jnp.zeros((8, channels), jnp.float32)
    squares = jnp.zeros((8, channels), jnp.float32)
    for f, r in loads:
        x = raw[frames + f, 1 + r].astype(jnp.float32).reshape(cols // 8, 8, channels)
        total = total + jnp.sum(x, axis=0)
        squares = squares + jnp.sum(x * x, axis=0)
    total = jnp.sum(total, axis=0, keepdims=True)
    squares = jnp.sum(squares, axis=0, keepdims=True)
    for k in range(parts):
        mine[k : k + 1, :] = total[:, k * lanes : (k + 1) * lanes]
        mine[parts + k : parts + k + 1, :] = squares[:, k * lanes : (k + 1) * lanes]

    when(member, pl.semaphore_wait, barrier, above_it + before_it + edges + onward)

    def give(other, c):
        send(mine, got1.at[y, core], s1.at[other, c], r1.at[y, core], column(other, c)).start()

    @pl.when(member)
    def _():
        for other in range(y_n - 1):
            @pl.when(other < y)
            def _():
                if other:
                    give(other, 0)
                else:
                    when(no(top), give, other, 0)
                give(other, 1)
        when(no(beside_leader), give, y, 1 - core)

    sends = (
        (down, no(bottom)),
        (along, no(last)),
        (down_next, all_of(core == 1, no(any_of(bottom, last)))),
        (up_next, any_of(to_leader, all_of(core == 1, no(any_of(top, last))))),
        (up, all_of(no(top), no(to_leader))),
    )
    along_ends = no(first)
    arrivals = (
        (down, no(top)),
        (up, no(bottom)),
        (along, no(first)),
        (down_next, no(any_of(top, first))),
        (up_next, no(any_of(bottom, first))),
    )

    def tell(device):
        return send(mine, late, s0, r0, device)

    @pl.when(leader)
    def _():
        for q in range(h_n // 2, 0, -1):
            for c in range(2):
                tell(in_row(q, c, 0)).start()
        down.start()
        tell(in_row(0, 1, 0)).start()
        for q in range(h_n // 2 + 1, h_n):
            for c in range(2):
                tell(in_row(q, c, 0)).start()
        signal(perm0, {"tm": 0, "height": 1})
        signal(perm0, {"tm": 1, "height": 0})

    def hand_on():
        when(no(top), down.wait_recv)
        when(all_of(all_of(core == 0, no(top)), no(to_leader)), down_again.start)

    def hand_on_up():
        when(no(bottom), up.wait_recv)
        when(all_of(all_of(core == 0, no(bottom)), member), up_again.start)

    @pl.when(member)
    def _():
        for other in range(h_n):
            sender = jnp.where(y == 0, 1, 0) if other == 0 else 0
            when(turn(other) < here_turn, signal, perm2.at[h], in_row(other, sender))

    @pl.when(member)
    def _():
        for copy, there in sends:
            when(there, copy.start)

    @pl.when(leader)
    def _():
        for other in range(1, y_n):
            tell(column(other, 0)).start()

    @pl.when(member)
    def _():
        def arrived(other, c):
            send(mine, mine, s1.at[0, 0], r1.at[other, c], at(0, 0)).wait_recv()

        when(beside_leader, got1.at[0, 0].__setitem__, Ellipsis, jnp.zeros_like(mine))
        when(no(beside_leader), arrived, y, 1 - core)
        pair[...] = mine[...] + got1[y, 1 - core]
        row[...] = pair[...]
        for other in range(1, y_n):
            @pl.when(other > y)
            def _():
                arrived(other, 0)
                arrived(other, 1)
                row[...] += got1[other, 0] + got1[other, 1]

                @pl.when(passes_on)
                def _():
                    for c in range(2):
                        send(pair, got1.at[y, 0], s1.at[other, c], r1.at[y, 0], column(other, c)).start()

        for other in range(y_n):
            @pl.when(other < y)
            def _():
                arrived(other, 0)
                row[...] += got1[other, 0]

        def pass_on(other, c):
            send(row, got2.at[h], s2.at[other, c], r2.at[h], in_row(other, c)).start()

        got2[h] = row[...]

        @pl.when(passes_on)
        def _():
            for other in sorted(range(h_n), key=turn):
                @pl.when(other != h)
                def _():
                    when(turn(other) > here_turn, pl.semaphore_wait, perm2.at[other], 2)
                    if other:
                        pass_on(other, 0)
                    else:
                        when(y > 0, pass_on, other, 0)
                    pass_on(other, 1)

        when(no(to_leader), hand_on)
        hand_on_up()

    weights.wait()

    @pl.loop(0, 9)
    def _(i):
        a, c = i // 3, lax.rem(i, 3)
        for k in range(0, channels, 64):
            g0, g1, g2 = (wbuf[a, b, c, k : k + 64].astype(jnp.float32) for b in range(3))
            even, odd = 0.5 * (g0 + g2), 0.5 * g1
            mixed[a, 0, c, k : k + 64] = (even + odd).astype(jnp.bfloat16)
            mixed[a, 1, c, k : k + 64] = (even - odd).astype(jnp.bfloat16)

    @pl.when(member)
    def _():
        @pl.when(to_leader)
        def _():
            pl.semaphore_wait(perm0, 1)
            up.start()

        for other in range(h_n):
            when(other != h, send(row, got2.at[other], s2.at[0, 0], r2.at[other], at(0, 0)).wait_recv)
        here = got2[0]
        for other in range(1, h_n):
            here = here + got2[other]
        row2[...] = here

        @pl.when(beside_leader)
        def _():
            pl.semaphore_wait(perm0, 1)
            send(row2, late, s0, r0, {"tm": 0, "height": 0}).start()

    @pl.when(leader)
    def _():
        row2[...] = mine[...]

    relays = all_of(member, y == 0)
    tell(at(0, 0)).wait_recv()

    @pl.when(relays)
    def _():
        for other in range(1, y_n):
            send(late, late, s4.at[other], r0, column(other, core)).start()

    for copy in smalls:
        copy.wait()
    when(along_ends, along.wait_recv)
    when(all_of(beside_leader, no(bottom)), down_beside.start)
    when(leader, hand_on_up)
    when(arrivals[4][1], up_next.wait_recv)
    here = row2[...] + late[...]

    per_group = channels // GROUPS
    high = here.astype(jnp.bfloat16)
    rest = here - high.astype(jnp.float32)
    middle = rest.astype(jnp.bfloat16)
    low = (rest - middle.astype(jnp.float32)).astype(jnp.bfloat16)
    same = (lax.broadcasted_iota(jnp.int32, (lanes, lanes), 0) // per_group
            == lax.broadcasted_iota(jnp.int32, (lanes, lanes), 1) // per_group)
    same = jnp.where(same, 1.0, 0.0).astype(jnp.bfloat16)
    spread = sum(jnp.dot(a, same, preferred_element_type=jnp.float32) for a in (low, middle, high))
    cells = tm_n * h_n * frames * rows * cols * per_group
    spread = spread * (1.0 / cells)
    mean = spread[:parts]
    var = jnp.maximum(spread[parts:] - mean * mean, 0.0)
    scale = lax.rsqrt(var + EPSILON)

    def flat(a):
        return jnp.concatenate([a[k : k + 1] for k in range(parts)], axis=1)

    half_scale = flat(scale) * gbuf[...].reshape(1, channels) * 0.5
    half_shift = hbuf[...].reshape(1, channels) * 0.5 - flat(mean) * half_scale

    step = 16

    def activated(f, r, k):
        source = jnp.where(first, frames, f) if f < frames else f
        v = raw[source, r, k : k + step].astype(jnp.float32) * half_scale + half_shift
        return v + v * jnp.tanh(v)

    def put(p, f, pair, k, value):
        act[p, f, pair, k : k + step] = value.astype(jnp.bfloat16)

    for f in range(2 * frames):
        for k in range(0, cols, step):
            d = [activated(f, r, k) for r in range(1, rows + 1)]
            for pair in range(2):
                put(1, f, pair, k, d[2 * pair] + d[2 * pair + 1])
                put(2, f, pair, k, d[2 * pair + 1] - d[2 * pair])
            put(0, f, 1, k, d[1] - d[3])
            kept[f, k : k + step] = d[1]
            put(3, f, 0, k, d[0] - d[2])
            below = jnp.where(bottom, 0.0, activated(f, rows + 1, k))
            put(3, f, 1, k, d[2] - below)

    m = frames * 2 * cols

    def product(p, c):
        acc = None
        for a in range(3):
            lhs = act[p, a : a + frames].reshape(m, channels)
            rhs = wbuf[a, 2 * (p // 3), c] if p in (0, 3) else mixed[a, p - 1, c]
            part = jnp.dot(lhs, rhs, preferred_element_type=jnp.float32)
            acc = part if acc is None else acc + part
        return acc

    for c in range(3):
        m1, m2 = product(1, c), product(2, c)
        sums[c, 0] = m1 + m2
        sums[c, 1] = m1 - m2

    when(to_leader, hand_on)
    when(arrivals[3][1], down_next.wait_recv)

    for f in range(2 * frames):
        for k in range(0, cols, step):
            above = jnp.where(top, 0.0, activated(f, 0, k))
            put(0, f, 0, k, above - kept[f, k : k + step])

    offset = bbuf[...].reshape(1, -1)
    for c in range(3):
        sums[c, 1] = sums[c, 1] - product(3, c)
        sums[c, 0] = sums[c, 0] + product(0, c)
    for odd in range(2):
        for f in range(frames):
            for pair in range(2):
                at0 = (f * 2 + pair) * cols
                left, middle, right = (sums[c, odd, at0 : at0 + cols] for c in range(3))
                zero = jnp.zeros_like(left[:1])
                left = jnp.concatenate([zero, left[:-1]], axis=0)
                right = jnp.concatenate([right[1:], zero], axis=0)
                out[f, 2 * pair + odd] = (middle + left + right + offset).astype(jnp.bfloat16)

    @pl.when(leader)
    def _():
        send(span, span, s0, r0, at(0, 0)).wait_send()

    @pl.when(relays)
    def _():
        for other in range(1, y_n):
            send(late, late, s4.at[other], r0, at(0, 0)).wait_send()

    when(beside_leader, send(row2, late, s0, r0, at(0, 0)).wait_send)

    @pl.when(member)
    def _():
        def left(sem):
            send(mine, mine, sem, r0, at(0, 0)).wait_send()

        when(no(beside_leader), left, s1.at[y, 1 - core])
        for other in range(y_n):
            for c in range(2):
                sent = any_of(other < y, all_of(other > y, passes_on))
                if not other and not c:
                    sent = all_of(sent, no(top))
                when(sent, left, s1.at[other, c])

        @pl.when(passes_on)
        def _():
            for other in range(h_n):
                for c in range(2):
                    sent = other != h if other or c else all_of(other != h, y > 0)
                    when(sent, left, s2.at[other, c])

    for copy, there in sends[:-1]:
        when(there, copy.wait_send)
    when(no(top), up.wait_send)
    when(all_of(all_of(core == 0, no(top)), no(to_leader)), down_again.wait_send)
    when(all_of(beside_leader, no(bottom)), down_beside.wait_send)
    when(all_of(all_of(core == 0, no(bottom)), member), up_again.wait_send)


def solution(mesh):
    sizes = (mesh.shape["tm"], mesh.shape["height"])

    def on_device(features, gain, shift, weight, bias):
        frames, rows, cols, channels = features.shape
        cout = weight.shape[-1]
        y_n, h_n = sizes[0] // 2, sizes[1]
        any_space = pl.BlockSpec(memory_space=pl.ANY)
        slab = (2 * frames, rows + 2, cols, channels)
        dma = pltpu.SemaphoreType.DMA
        return pl.pallas_call(
            functools.partial(kernel, sizes),
            out_shape=pltpu.VMEM((frames, rows, cols, cout), jnp.bfloat16),
            in_specs=[any_space] * 5,
            out_specs=pl.BlockSpec(memory_space=pltpu.VMEM),
            scratch_shapes=[
                pltpu.VMEM(slab, jnp.bfloat16),
                pltpu.VMEM((4, 2 * frames, 2, cols, channels), jnp.bfloat16),
                pltpu.VMEM(weight.shape, jnp.bfloat16),
                pltpu.VMEM((3, 2, 3, channels, cout), jnp.bfloat16),
                pltpu.VMEM((3, 2, frames * 2 * cols, cout), jnp.float32),
                pltpu.VMEM((2 * frames, cols, channels), jnp.float32),
                pltpu.VMEM((channels,), jnp.float32),
                pltpu.VMEM((channels,), jnp.float32),
                pltpu.VMEM((cout,), jnp.float32),
                *[pltpu.VMEM((8, 128), jnp.float32)] * 5,
                pltpu.VMEM((2 * h_n - 1 + y_n - 1, 8, 128), jnp.float32),
                pltpu.VMEM((y_n, 2, 8, 128), jnp.float32),
                pltpu.VMEM((h_n, 8, 128), jnp.float32),
                dma((frames, rows)), dma((3,)), dma, dma, dma, dma((y_n, 2)), dma((y_n, 2)),
                dma((h_n, 2)), dma((h_n,)), dma((y_n,)), dma, dma((5,)), dma((5,)),
                pltpu.SemaphoreType.REGULAR, pltpu.SemaphoreType.REGULAR((h_n,)),
            ],
            compiler_params=pltpu.CompilerParams(
                collective_id=0, has_side_effects=True, vmem_limit_bytes=60 * 1024 * 1024
            ),
        )(features, gain, shift, weight, bias)

    return jax.shard_map(
        on_device,
        mesh=mesh,
        in_specs=(P(("clips", "tm"), "height", None, None), P(), P(), P(), P()),
        out_specs=P(("clips", "tm"), "height", None, None),
        check_vma=False,
    )
```

```python
import functools

import jax
import jax.numpy as jnp
from jax import lax
from jax.experimental import pallas as pl
from jax.experimental.pallas import tpu as pltpu
from jax.sharding import PartitionSpec as P

MESH = pl.DeviceIdType.MESH
GROUPS = 32
EPSILON = 1e-06


def kernel(sizes, feat, gain, shift, weight, bias, out, raw, act, wbuf, mixed, sums, kept, gbuf, hbuf, bbuf,
           mine, pair, row, row2, late, span, got1, got2, in_sem, small_sem, w_sem, s0, r0, s1, r1, s2, r2, s4, s5, hs, hr, perm0, perm2):
    tm_n, h_n = sizes
    y_n = tm_n // 2
    frames, rows, cols, channels = feat.shape
    loads = {}
    for f in range(frames):
        for r in range(rows):
            loads[f, r] = pltpu.make_async_copy(feat.at[f, r], raw.at[frames + f, 1 + r], in_sem.at[f, r])
            loads[f, r].start()
    smalls = [pltpu.make_async_copy(a, b, small_sem.at[i])
              for i, (a, b) in enumerate(((gain, gbuf), (shift, hbuf), (bias, bbuf)))]
    for copy in smalls:
        copy.start()
    weights = pltpu.make_async_copy(weight, wbuf, w_sem)

    lanes = 128
    parts = channels // lanes
    tm = lax.axis_index("tm")
    h = lax.axis_index("height")
    core = lax.rem(tm, 2)
    y = lax.div(tm, 2)
    first, last = tm == 0, tm == tm_n - 1
    top, bottom = h == 0, h == h_n - 1

    wide = 2 * h_n
    leader = jnp.logical_and(first, top)
    member = jnp.logical_not(leader)
    all_of, any_of, no = jnp.logical_and, jnp.logical_or, jnp.logical_not
    beside_leader = all_of(tm == 1, top)
    passes_on = any_of(all_of(core == 0, member), beside_leader)
    receives_along = all_of(core == 0, no(first))
    relays = all_of(core == 1, y == 0)
    to_leader = all_of(first, h == 1)

    def at(dtm, dh):
        return {"tm": tm + dtm, "height": h + dh}

    def in_row(other, c, chip=y):
        return {"tm": chip * 2 + c, "height": other}

    def column(other, c):
        return {"tm": other * 2 + c, "height": h}

    def turn(v):
        half = h_n // 2
        if isinstance(v, int):
            return v if v < half else half + h_n - 1 - v
        return jnp.where(v < half, v, half + h_n - 1 - v)

    here_turn = turn(h)
    def when(condition, f, *args):
        pl.when(condition)(functools.partial(f, *args))

    def signal(sem, device):
        pl.semaphore_signal(sem, inc=1, device_id=device, device_id_type=MESH)

    def send(src, dst, s, r, device):
        return pltpu.make_async_remote_copy(src_ref=src, dst_ref=dst, send_sem=s, recv_sem=r,
                                            device_id=device, device_id_type=MESH)

    barrier = pltpu.get_barrier_semaphore()

    @pl.when(member)
    def _():
        for other in sorted(range(1, h_n), key=lambda q: -turn(q)):
            @pl.when(turn(other) > here_turn)
            def _():
                signal(barrier, in_row(other, 0))
                signal(barrier, in_row(other, 1))
        when(no(beside_leader), signal, barrier, column(y, 1 - core))
        when(no(top), signal, barrier, at(0, -1))
        when(no(bottom), signal, barrier, at(0, 1))

        @pl.when(receives_along)
        def _():
            signal(barrier, at(-1, 0))
            when(no(top), signal, barrier, at(-1, -1))
            when(no(bottom), signal, barrier, at(-1, 1))

        when(any_of(y == 0, all_of(core == 0, top)), signal, barrier, {"tm": 0, "height": 0})
        for other in range(1, y_n):
            @pl.when(other > y)
            def _():
                signal(barrier, column(other, 0))
                signal(barrier, column(other, 1))

    def number(condition):
        return condition.astype(jnp.int32)

    above_it = 2 * y - number(all_of(top, y > 0)) + 1 - number(beside_leader)
    before_it = 2 * here_turn - number(all_of(y == 0, h > 0))
    edges = number(no(bottom)) + number(no(top)) - number(to_leader)
    onward = number(all_of(core == 1, no(last))) * (3 - number(top) - number(bottom))
    for_leader = (wide - 1) + (y_n - 1) + 1
    def edge(src_row, dst_row, frame, dtm, dh, i):
        return send(raw.at[frames:, src_row], raw.at[pl.ds(frame, frames), dst_row],
                    hs.at[i], hr.at[i], at(dtm, dh))

    down = edge(rows, 0, frames, 0, 1, 0)
    up = edge(1, rows + 1, frames, 0, -1, 1)
    down_next = edge(rows, 0, 0, 1, 1, 2)
    up_next = edge(1, rows + 1, 0, 1, -1, 3)
    along = send(raw.at[frames:, 1 : 1 + rows], raw.at[:frames, 1 : 1 + rows], hs.at[4], hr.at[4],
                 at(1, 0))
    down_again = edge(0, 0, 0, 1, 0, 2)
    up_again = edge(rows + 1, rows + 1, 0, 1, 0, 3)
    down_beside = send(raw.at[:frames, rows], raw.at[:frames, 0], s5, hr.at[2], at(0, 1))
    total = jnp.zeros((8, channels), jnp.float32)
    squares = jnp.zeros((8, channels), jnp.float32)
    for f, r in loads:
        loads[f, r].wait()
        x = raw[frames + f, 1 + r].astype(jnp.float32).reshape(cols // 8, 8, channels)
        total = total + jnp.sum(x, axis=0)
        squares = squares + jnp.sum(x * x, axis=0)
    weights.start()
    total = jnp.sum(total, axis=0, keepdims=True)
    squares = jnp.sum(squares, axis=0, keepdims=True)
    for k in range(parts):
        mine[k : k + 1, :] = total[:, k * lanes : (k + 1) * lanes]
        mine[parts + k : parts + k + 1, :] = squares[:, k * lanes : (k + 1) * lanes]

    pl.semaphore_wait(barrier, jnp.where(leader, for_leader, above_it + before_it + edges + onward))

    def give(other, c):
        send(mine, got1.at[y, core], s1.at[other, c], r1.at[y, core], column(other, c)).start()

    @pl.when(member)
    def _():
        for other in range(y_n - 1):
            @pl.when(other < y)
            def _():
                if other:
                    give(other, 0)
                else:
                    when(no(top), give, other, 0)
                give(other, 1)
        when(no(beside_leader), give, y, 1 - core)

    sends = (
        (down, no(bottom)),
        (along, no(last)),
        (down_next, all_of(core == 1, no(any_of(bottom, last)))),
        (up_next, any_of(to_leader, all_of(core == 1, no(any_of(top, last))))),
        (up, all_of(no(top), no(to_leader))),
    )
    along_ends = all_of(no(first), any_of(no(beside_leader), bottom))
    arrivals = (
        (down, no(top)),
        (up, no(bottom)),
        (along, no(first)),
        (down_next, no(any_of(top, first))),
        (up_next, no(any_of(bottom, first))),
    )

    def tell(device):
        return send(mine, late, s0, r0, device)

    @pl.when(leader)
    def _():
        for q in sorted(range(h_n), key=lambda q: -min(q, h_n - q)):
            for c in range(2):
                if q or c:
                    tell(in_row(q, c, 0)).start()
        along.start()
        down.start()
        signal(perm0, {"tm": 0, "height": 1})
        signal(perm0, {"tm": 1, "height": 0})

    def hand_on():
        when(no(top), down.wait_recv)
        when(all_of(all_of(core == 0, no(top)), no(to_leader)), down_again.start)

    def hand_on_up():
        when(no(bottom), up.wait_recv)
        when(all_of(all_of(core == 0, no(bottom)), member), up_again.start)

    @pl.when(member)
    def _():
        for other in range(h_n):
            when(turn(other) < here_turn, signal, perm2.at[h], in_row(other, 1))

    @pl.when(member)
    def _():
        for copy, there in sends:
            when(there, copy.start)

    @pl.when(leader)
    def _():
        for other in range(1, y_n):
            tell(column(other, 0)).start()

    @pl.when(member)
    def _():
        def arrived(other, c):
            send(mine, mine, s1.at[0, 0], r1.at[other, c], at(0, 0)).wait_recv()

        when(beside_leader, got1.at[0, 0].__setitem__, Ellipsis, jnp.zeros_like(mine))
        when(no(beside_leader), arrived, y, 1 - core)
        pair[...] = mine[...] + got1[y, 1 - core]
        row[...] = pair[...]
        for other in range(1, y_n):
            @pl.when(other > y)
            def _():
                arrived(other, 0)
                arrived(other, 1)
                row[...] += got1[other, 0] + got1[other, 1]

                @pl.when(passes_on)
                def _():
                    for c in range(2):
                        send(pair, got1.at[y, 0], s1.at[other, c], r1.at[y, 0], column(other, c)).start()

        for other in range(y_n):
            @pl.when(other < y)
            def _():
                arrived(other, 0)
                row[...] += got1[other, 0]

        def pass_on(other, c):
            send(row, got2.at[h], s2.at[other, c], r2.at[h], in_row(other, c)).start()

        got2[h] = row[...]

        @pl.when(core == 1)
        def _():
            for other in sorted(range(h_n), key=turn):
                @pl.when(other != h)
                def _():
                    when(turn(other) > here_turn, pl.semaphore_wait, perm2.at[other], 2)
                    if other:
                        pass_on(other, 0)
                    else:
                        when(y > 0, pass_on, other, 0)
                    pass_on(other, 1)

        when(no(to_leader), hand_on)
        hand_on_up()

    weights.wait()

    @pl.loop(0, 9)
    def _(i):
        a, c = i // 3, lax.rem(i, 3)
        for k in range(0, channels, 64):
            g0, g1, g2 = (wbuf[a, b, c, k : k + 64].astype(jnp.float32) for b in range(3))
            even, odd = 0.5 * (g0 + g2), 0.5 * g1
            mixed[a, 0, c, k : k + 64] = (even + odd).astype(jnp.bfloat16)
            mixed[a, 1, c, k : k + 64] = (even - odd).astype(jnp.bfloat16)

    @pl.when(member)
    def _():
        @pl.when(to_leader)
        def _():
            pl.semaphore_wait(perm0, 1)
            up.start()

        @pl.when(all_of(beside_leader, no(bottom)))
        def _():
            along.wait_recv()
            down_beside.start()

        @pl.when(relays)
        def _():
            tell(at(0, 0)).wait_recv()
            for other in range(1, y_n):
                when(no(top), send(late, late, s4.at[other, 0], r0, column(other, 0)).start)
                send(late, late, s4.at[other, 1], r0, column(other, 1)).start()

        for other in range(h_n):
            when(other != h, send(row, got2.at[other], s2.at[0, 0], r2.at[other], at(0, 0)).wait_recv)
        here = got2[0]
        for other in range(1, h_n):
            here = here + got2[other]
        row2[...] = here

        @pl.when(beside_leader)
        def _():
            pl.semaphore_wait(perm0, 1)
            send(row2, late, s0, r0, {"tm": 0, "height": 0}).start()

    @pl.when(leader)
    def _():
        row2[...] = mine[...]

    when(no(relays), tell(at(0, 0)).wait_recv)

    for copy in smalls:
        copy.wait()
    when(along_ends, along.wait_recv)
    when(leader, hand_on_up)
    when(arrivals[4][1], up_next.wait_recv)
    here = row2[...] + late[...]

    per_group = channels // GROUPS
    high = here.astype(jnp.bfloat16)
    rest = here - high.astype(jnp.float32)
    middle = rest.astype(jnp.bfloat16)
    low = (rest - middle.astype(jnp.float32)).astype(jnp.bfloat16)
    same = (lax.broadcasted_iota(jnp.int32, (lanes, lanes), 0) // per_group
            == lax.broadcasted_iota(jnp.int32, (lanes, lanes), 1) // per_group)
    same = jnp.where(same, 1.0, 0.0).astype(jnp.bfloat16)
    spread = sum(jnp.dot(a, same, preferred_element_type=jnp.float32) for a in (low, middle, high))
    cells = tm_n * h_n * frames * rows * cols * per_group
    spread = spread * (1.0 / cells)
    mean = spread[:parts]
    var = jnp.maximum(spread[parts:] - mean * mean, 0.0)
    scale = lax.rsqrt(var + EPSILON)

    def flat(a):
        return jnp.concatenate([a[k : k + 1] for k in range(parts)], axis=1)

    half_scale = flat(scale) * gbuf[...].reshape(1, channels) * 0.5
    half_shift = hbuf[...].reshape(1, channels) * 0.5 - flat(mean) * half_scale

    step = 16

    def activated(f, r, k):
        source = jnp.where(first, frames, f) if f < frames else f
        v = raw[source, r, k : k + step].astype(jnp.float32) * half_scale + half_shift
        return v + v * jnp.tanh(v)

    def put(p, f, pair, k, value):
        act[p, f, pair, k : k + step] = value.astype(jnp.bfloat16)

    for f in range(2 * frames):
        for k in range(0, cols, step):
            d = [activated(f, r, k) for r in range(1, rows + 1)]
            for pair in range(2):
                put(1, f, pair, k, d[2 * pair] + d[2 * pair + 1])
                put(2, f, pair, k, d[2 * pair + 1] - d[2 * pair])
            put(0, f, 1, k, d[1] - d[3])
            kept[f, k : k + step] = d[1]
            put(3, f, 0, k, d[0] - d[2])
            below = jnp.where(bottom, 0.0, activated(f, rows + 1, k))
            put(3, f, 1, k, d[2] - below)

    m = frames * 2 * cols

    def product(p, c):
        acc = None
        for a in range(3):
            lhs = act[p, a : a + frames].reshape(m, channels)
            rhs = wbuf[a, 2 * (p // 3), c] if p in (0, 3) else mixed[a, p - 1, c]
            part = jnp.dot(lhs, rhs, preferred_element_type=jnp.float32)
            acc = part if acc is None else acc + part
        return acc

    for c in range(3):
        m1, m2 = product(1, c), product(2, c)
        sums[c, 0] = m1 + m2
        sums[c, 1] = m1 - m2

    when(to_leader, hand_on)
    when(arrivals[3][1], down_next.wait_recv)

    for f in range(2 * frames):
        for k in range(0, cols, step):
            above = jnp.where(top, 0.0, activated(f, 0, k))
            put(0, f, 0, k, above - kept[f, k : k + step])

    offset = bbuf[...].reshape(1, -1)
    for c in range(3):
        sums[c, 1] = sums[c, 1] - product(3, c)
        sums[c, 0] = sums[c, 0] + product(0, c)
    for odd in range(2):
        for f in range(frames):
            for pair in range(2):
                at0 = (f * 2 + pair) * cols
                left, middle, right = (sums[c, odd, at0 : at0 + cols] for c in range(3))
                zero = jnp.zeros_like(left[:1])
                left = jnp.concatenate([zero, left[:-1]], axis=0)
                right = jnp.concatenate([right[1:], zero], axis=0)
                out[f, 2 * pair + odd] = (middle + left + right + offset).astype(jnp.bfloat16)

    @pl.when(leader)
    def _():
        send(span, span, s0, r0, at(0, 0)).wait_send()

    @pl.when(relays)
    def _():
        for other in range(1, y_n):
            when(no(top), send(late, late, s4.at[other, 0], r0, at(0, 0)).wait_send)
            send(late, late, s4.at[other, 1], r0, at(0, 0)).wait_send()

    when(beside_leader, send(row2, late, s0, r0, at(0, 0)).wait_send)

    @pl.when(member)
    def _():
        def left(sem):
            send(mine, mine, sem, r0, at(0, 0)).wait_send()

        when(no(beside_leader), left, s1.at[y, 1 - core])
        for other in range(y_n):
            for c in range(2):
                sent = any_of(other < y, all_of(other > y, passes_on))
                if not other and not c:
                    sent = all_of(sent, no(top))
                when(sent, left, s1.at[other, c])

        @pl.when(core == 1)
        def _():
            for other in range(h_n):
                for c in range(2):
                    sent = other != h if other or c else all_of(other != h, y > 0)
                    when(sent, left, s2.at[other, c])

    for copy, there in sends[:-1]:
        when(there, copy.wait_send)
    when(no(top), up.wait_send)
    when(all_of(all_of(core == 0, no(top)), no(to_leader)), down_again.wait_send)
    when(all_of(beside_leader, no(bottom)), down_beside.wait_send)
    when(all_of(all_of(core == 0, no(bottom)), member), up_again.wait_send)


def solution(mesh):
    sizes = (mesh.shape["tm"], mesh.shape["height"])

    def on_device(features, gain, shift, weight, bias):
        frames, rows, cols, channels = features.shape
        cout = weight.shape[-1]
        y_n, h_n = sizes[0] // 2, sizes[1]
        any_space = pl.BlockSpec(memory_space=pl.ANY)
        slab = (2 * frames, rows + 2, cols, channels)
        dma = pltpu.SemaphoreType.DMA
        return pl.pallas_call(
            functools.partial(kernel, sizes),
            out_shape=pltpu.VMEM((frames, rows, cols, cout), jnp.bfloat16),
            in_specs=[any_space] * 5,
            out_specs=pl.BlockSpec(memory_space=pltpu.VMEM),
            scratch_shapes=[
                pltpu.VMEM(slab, jnp.bfloat16),
                pltpu.VMEM((4, 2 * frames, 2, cols, channels), jnp.bfloat16),
                pltpu.VMEM(weight.shape, jnp.bfloat16),
                pltpu.VMEM((3, 2, 3, channels, cout), jnp.bfloat16),
                pltpu.VMEM((3, 2, frames * 2 * cols, cout), jnp.float32),
                pltpu.VMEM((2 * frames, cols, channels), jnp.float32),
                pltpu.VMEM((channels,), jnp.float32),
                pltpu.VMEM((channels,), jnp.float32),
                pltpu.VMEM((cout,), jnp.float32),
                *[pltpu.VMEM((8, 128), jnp.float32)] * 5,
                pltpu.VMEM((2 * h_n - 1 + y_n - 1, 8, 128), jnp.float32),
                pltpu.VMEM((y_n, 2, 8, 128), jnp.float32),
                pltpu.VMEM((h_n, 8, 128), jnp.float32),
                dma((frames, rows)), dma((3,)), dma, dma, dma, dma((y_n, 2)), dma((y_n, 2)),
                dma((h_n, 2)), dma((h_n,)), dma((y_n, 2)), dma, dma((7,)), dma((7,)),
                pltpu.SemaphoreType.REGULAR, pltpu.SemaphoreType.REGULAR((h_n,)),
            ],
            compiler_params=pltpu.CompilerParams(
                collective_id=0, has_side_effects=True, vmem_limit_bytes=60 * 1024 * 1024
            ),
        )(features, gain, shift, weight, bias)

    return jax.shard_map(
        on_device,
        mesh=mesh,
        in_specs=(P(("clips", "tm"), "height", None, None), P(), P(), P(), P()),
        out_specs=P(("clips", "tm"), "height", None, None),
        check_vma=False,
    )
```

```python
import functools

import jax
import jax.numpy as jnp
from jax import lax
from jax.experimental import pallas as pl
from jax.experimental.pallas import tpu as pltpu
from jax.sharding import PartitionSpec as P

MESH = pl.DeviceIdType.MESH
GROUPS = 32
EPSILON = 1e-06


def kernel(sizes, feat, gain, shift, weight, bias, out, raw, act, wbuf, mixed, sums, kept, gbuf, hbuf, bbuf,
           mine, pair, row, row2, late, span, got1, got2, in_sem, small_sem, w_sem, s0, r0, s1, r1, s2, r2, s4, s5, hs, hr, perm0, perm2):
    tm_n, h_n = sizes
    y_n = tm_n // 2
    frames, rows, cols, channels = feat.shape
    loads = {}
    for f in range(frames):
        for r in range(rows):
            loads[f, r] = pltpu.make_async_copy(feat.at[f, r], raw.at[frames + f, 1 + r], in_sem.at[f, r])
            loads[f, r].start()
    smalls = [pltpu.make_async_copy(a, b, small_sem.at[i])
              for i, (a, b) in enumerate(((gain, gbuf), (shift, hbuf), (bias, bbuf)))]
    for copy in smalls:
        copy.start()
    weights = pltpu.make_async_copy(weight, wbuf, w_sem)

    lanes = 128
    parts = channels // lanes
    tm = lax.axis_index("tm")
    h = lax.axis_index("height")
    core = lax.rem(tm, 2)
    y = lax.div(tm, 2)
    first, last = tm == 0, tm == tm_n - 1
    top, bottom = h == 0, h == h_n - 1

    wide = 2 * h_n
    leader = jnp.logical_and(first, top)
    member = jnp.logical_not(leader)
    all_of, any_of, no = jnp.logical_and, jnp.logical_or, jnp.logical_not
    beside_leader = all_of(tm == 1, top)
    passes_on = any_of(all_of(core == 0, member), beside_leader)
    receives_along = all_of(core == 0, no(first))
    to_leader = all_of(first, h == 1)

    def at(dtm, dh):
        return {"tm": tm + dtm, "height": h + dh}

    def in_row(other, c, chip=y):
        return {"tm": chip * 2 + c, "height": other}

    def column(other, c):
        return {"tm": other * 2 + c, "height": h}

    def turn(v):
        half = h_n // 2
        if isinstance(v, int):
            return v if v < half else half + h_n - 1 - v
        return jnp.where(v < half, v, half + h_n - 1 - v)

    here_turn = turn(h)
    def when(condition, f, *args):
        pl.when(condition)(functools.partial(f, *args))

    def signal(sem, device):
        pl.semaphore_signal(sem, inc=1, device_id=device, device_id_type=MESH)

    def send(src, dst, s, r, device):
        return pltpu.make_async_remote_copy(src_ref=src, dst_ref=dst, send_sem=s, recv_sem=r,
                                            device_id=device, device_id_type=MESH)

    barrier = pltpu.get_barrier_semaphore()

    @pl.when(member)
    def _():
        for other in range(1, h_n):
            @pl.when(turn(other) > here_turn)
            def _():
                signal(barrier, in_row(other, 0))
                signal(barrier, in_row(other, 1))
        when(no(beside_leader), signal, barrier, column(y, 1 - core))
        when(no(top), signal, barrier, at(0, -1))
        when(no(bottom), signal, barrier, at(0, 1))

        @pl.when(receives_along)
        def _():
            signal(barrier, at(-1, 0))
            when(no(top), signal, barrier, at(-1, -1))
            when(no(bottom), signal, barrier, at(-1, 1))

        when(any_of(y == 0, all_of(core == 0, top)), signal, barrier, {"tm": 0, "height": 0})
        for other in range(1, y_n):
            @pl.when(other > y)
            def _():
                signal(barrier, column(other, 0))
                signal(barrier, column(other, 1))

    def number(condition):
        return condition.astype(jnp.int32)

    above_it = 2 * y - number(all_of(top, y > 0)) + 1 - number(beside_leader)
    before_it = 2 * here_turn - number(all_of(y == 0, h > 0))
    edges = number(no(bottom)) + number(no(top)) - number(to_leader)
    onward = number(all_of(core == 1, no(last))) * (3 - number(top) - number(bottom))
    for_leader = (wide - 1) + (y_n - 1) + 1
    def edge(src_row, dst_row, frame, dtm, dh, i):
        return send(raw.at[frames:, src_row], raw.at[pl.ds(frame, frames), dst_row],
                    hs.at[i], hr.at[i], at(dtm, dh))

    down = edge(rows, 0, frames, 0, 1, 0)
    up = edge(1, rows + 1, frames, 0, -1, 1)
    down_next = edge(rows, 0, 0, 1, 1, 2)
    up_next = edge(1, rows + 1, 0, 1, -1, 3)
    along = send(raw.at[frames:, 1 : 1 + rows], raw.at[:frames, 1 : 1 + rows], hs.at[4], hr.at[4],
                 at(1, 0))
    down_again = edge(0, 0, 0, 1, 0, 2)
    up_again = edge(rows + 1, rows + 1, 0, 1, 0, 3)
    down_beside = send(raw.at[:frames, rows], raw.at[:frames, 0], s5, hr.at[2], at(0, 1))
    total = jnp.zeros((8, channels), jnp.float32)
    squares = jnp.zeros((8, channels), jnp.float32)
    for f, r in loads:
        loads[f, r].wait()
        x = raw[frames + f, 1 + r].astype(jnp.float32).reshape(cols // 8, 8, channels)
        total = total + jnp.sum(x, axis=0)
        squares = squares + jnp.sum(x * x, axis=0)
    weights.start()
    total = jnp.sum(total, axis=0, keepdims=True)
    squares = jnp.sum(squares, axis=0, keepdims=True)
    for k in range(parts):
        mine[k : k + 1, :] = total[:, k * lanes : (k + 1) * lanes]
        mine[parts + k : parts + k + 1, :] = squares[:, k * lanes : (k + 1) * lanes]

    pl.semaphore_wait(barrier, jnp.where(leader, for_leader, above_it + before_it + edges + onward))

    def give(other, c):
        send(mine, got1.at[y, core], s1.at[other, c], r1.at[y, core], column(other, c)).start()

    @pl.when(member)
    def _():
        for other in range(y_n - 1):
            @pl.when(other < y)
            def _():
                if other:
                    give(other, 0)
                else:
                    when(no(top), give, other, 0)
                give(other, 1)
        when(no(beside_leader), give, y, 1 - core)

    sends = (
        (down, no(bottom)),
        (along, no(last)),
        (down_next, all_of(core == 1, no(any_of(bottom, last)))),
        (up_next, any_of(to_leader, all_of(core == 1, no(any_of(top, last))))),
        (up, all_of(no(top), no(to_leader))),
    )
    along_ends = all_of(no(first), any_of(no(beside_leader), bottom))
    arrivals = (
        (down, no(top)),
        (up, no(bottom)),
        (along, no(first)),
        (down_next, no(any_of(top, first))),
        (up_next, no(any_of(bottom, first))),
    )

    def tell(device):
        return send(mine, late, s0, r0, device)

    @pl.when(leader)
    def _():
        for q in sorted(range(h_n), key=lambda q: -min(q, h_n - q)):
            for c in range(2):
                if q or c:
                    tell(in_row(q, c, 0)).start()
        along.start()
        down.start()
        signal(perm0, {"tm": 0, "height": 1})
        signal(perm0, {"tm": 1, "height": 0})

    def hand_on():
        when(no(top), down.wait_recv)
        when(all_of(all_of(core == 0, no(top)), no(to_leader)), down_again.start)

    def hand_on_up():
        when(no(bottom), up.wait_recv)
        when(all_of(all_of(core == 0, no(bottom)), member), up_again.start)

    @pl.when(member)
    def _():
        for other in range(h_n):
            sender = jnp.where(y == 0, 1, 0) if other == 0 else 0
            when(turn(other) < here_turn, signal, perm2.at[h], in_row(other, sender))

    @pl.when(member)
    def _():
        for copy, there in sends:
            when(there, copy.start)

    @pl.when(leader)
    def _():
        for other in range(1, y_n):
            tell(column(other, 0)).start()

    @pl.when(member)
    def _():
        def arrived(other, c):
            send(mine, mine, s1.at[0, 0], r1.at[other, c], at(0, 0)).wait_recv()

        when(beside_leader, got1.at[0, 0].__setitem__, Ellipsis, jnp.zeros_like(mine))
        when(no(beside_leader), arrived, y, 1 - core)
        pair[...] = mine[...] + got1[y, 1 - core]
        row[...] = pair[...]
        for other in range(1, y_n):
            @pl.when(other > y)
            def _():
                arrived(other, 0)
                arrived(other, 1)
                row[...] += got1[other, 0] + got1[other, 1]

                @pl.when(passes_on)
                def _():
                    for c in range(2):
                        send(pair, got1.at[y, 0], s1.at[other, c], r1.at[y, 0], column(other, c)).start()

        for other in range(y_n):
            @pl.when(other < y)
            def _():
                arrived(other, 0)
                row[...] += got1[other, 0]

        def pass_on(other, c):
            send(row, got2.at[h], s2.at[other, c], r2.at[h], in_row(other, c)).start()

        got2[h] = row[...]

        @pl.when(passes_on)
        def _():
            for other in sorted(range(h_n), key=turn):
                @pl.when(other != h)
                def _():
                    when(turn(other) > here_turn, pl.semaphore_wait, perm2.at[other], 2)
                    if other:
                        pass_on(other, 0)
                    else:
                        when(y > 0, pass_on, other, 0)
                    pass_on(other, 1)

        when(no(to_leader), hand_on)
        hand_on_up()

    weights.wait()

    @pl.loop(0, 9)
    def _(i):
        a, c = i // 3, lax.rem(i, 3)
        for k in range(0, channels, 64):
            g0, g1, g2 = (wbuf[a, b, c, k : k + 64].astype(jnp.float32) for b in range(3))
            even, odd = 0.5 * (g0 + g2), 0.5 * g1
            mixed[a, 0, c, k : k + 64] = (even + odd).astype(jnp.bfloat16)
            mixed[a, 1, c, k : k + 64] = (even - odd).astype(jnp.bfloat16)

    @pl.when(member)
    def _():
        @pl.when(to_leader)
        def _():
            pl.semaphore_wait(perm0, 1)
            up.start()

        @pl.when(all_of(beside_leader, no(bottom)))
        def _():
            along.wait_recv()
            down_beside.start()

        for other in range(h_n):
            when(other != h, send(row, got2.at[other], s2.at[0, 0], r2.at[other], at(0, 0)).wait_recv)
        here = got2[0]
        for other in range(1, h_n):
            here = here + got2[other]
        row2[...] = here

        @pl.when(beside_leader)
        def _():
            pl.semaphore_wait(perm0, 1)
            send(row2, late, s0, r0, {"tm": 0, "height": 0}).start()

    @pl.when(leader)
    def _():
        row2[...] = mine[...]

    relays = all_of(member, y == 0)
    tell(at(0, 0)).wait_recv()

    @pl.when(relays)
    def _():
        for other in range(1, y_n):
            send(late, late, s4.at[other], r0, column(other, core)).start()

    for copy in smalls:
        copy.wait()
    when(along_ends, along.wait_recv)
    when(leader, hand_on_up)
    when(arrivals[4][1], up_next.wait_recv)
    here = row2[...] + late[...]

    per_group = channels // GROUPS
    high = here.astype(jnp.bfloat16)
    rest = here - high.astype(jnp.float32)
    middle = rest.astype(jnp.bfloat16)
    low = (rest - middle.astype(jnp.float32)).astype(jnp.bfloat16)
    same = (lax.broadcasted_iota(jnp.int32, (lanes, lanes), 0) // per_group
            == lax.broadcasted_iota(jnp.int32, (lanes, lanes), 1) // per_group)
    same = jnp.where(same, 1.0, 0.0).astype(jnp.bfloat16)
    spread = sum(jnp.dot(a, same, preferred_element_type=jnp.float32) for a in (low, middle, high))
    cells = tm_n * h_n * frames * rows * cols * per_group
    spread = spread * (1.0 / cells)
    mean = spread[:parts]
    var = jnp.maximum(spread[parts:] - mean * mean, 0.0)
    scale = lax.rsqrt(var + EPSILON)

    def flat(a):
        return jnp.concatenate([a[k : k + 1] for k in range(parts)], axis=1)

    half_scale = flat(scale) * gbuf[...].reshape(1, channels) * 0.5
    half_shift = hbuf[...].reshape(1, channels) * 0.5 - flat(mean) * half_scale

    step = 16

    def activated(f, r, k):
        source = jnp.where(first, frames, f) if f < frames else f
        v = raw[source, r, k : k + step].astype(jnp.float32) * half_scale + half_shift
        return v + v * jnp.tanh(v)

    def put(p, f, pair, k, value):
        act[p, f, pair, k : k + step] = value.astype(jnp.bfloat16)

    for f in range(2 * frames):
        for k in range(0, cols, step):
            d = [activated(f, r, k) for r in range(1, rows + 1)]
            for pair in range(2):
                put(1, f, pair, k, d[2 * pair] + d[2 * pair + 1])
                put(2, f, pair, k, d[2 * pair + 1] - d[2 * pair])
            put(0, f, 1, k, d[1] - d[3])
            kept[f, k : k + step] = d[1]
            put(3, f, 0, k, d[0] - d[2])
            below = jnp.where(bottom, 0.0, activated(f, rows + 1, k))
            put(3, f, 1, k, d[2] - below)

    m = frames * 2 * cols

    def product(p, c):
        acc = None
        for a in range(3):
            lhs = act[p, a : a + frames].reshape(m, channels)
            rhs = wbuf[a, 2 * (p // 3), c] if p in (0, 3) else mixed[a, p - 1, c]
            part = jnp.dot(lhs, rhs, preferred_element_type=jnp.float32)
            acc = part if acc is None else acc + part
        return acc

    for c in range(3):
        m1, m2 = product(1, c), product(2, c)
        sums[c, 0] = m1 + m2
        sums[c, 1] = m1 - m2

    when(to_leader, hand_on)
    when(arrivals[3][1], down_next.wait_recv)

    for f in range(2 * frames):
        for k in range(0, cols, step):
            above = jnp.where(top, 0.0, activated(f, 0, k))
            put(0, f, 0, k, above - kept[f, k : k + step])

    offset = bbuf[...].reshape(1, -1)
    for c in range(3):
        sums[c, 1] = sums[c, 1] - product(3, c)
        sums[c, 0] = sums[c, 0] + product(0, c)
    for odd in range(2):
        for f in range(frames):
            for pair in range(2):
                at0 = (f * 2 + pair) * cols
                left, middle, right = (sums[c, odd, at0 : at0 + cols] for c in range(3))
                zero = jnp.zeros_like(left[:1])
                left = jnp.concatenate([zero, left[:-1]], axis=0)
                right = jnp.concatenate([right[1:], zero], axis=0)
                out[f, 2 * pair + odd] = (middle + left + right + offset).astype(jnp.bfloat16)

    @pl.when(leader)
    def _():
        send(span, span, s0, r0, at(0, 0)).wait_send()

    @pl.when(relays)
    def _():
        for other in range(1, y_n):
            send(late, late, s4.at[other], r0, at(0, 0)).wait_send()

    when(beside_leader, send(row2, late, s0, r0, at(0, 0)).wait_send)

    @pl.when(member)
    def _():
        def left(sem):
            send(mine, mine, sem, r0, at(0, 0)).wait_send()

        when(no(beside_leader), left, s1.at[y, 1 - core])
        for other in range(y_n):
            for c in range(2):
                sent = any_of(other < y, all_of(other > y, passes_on))
                if not other and not c:
                    sent = all_of(sent, no(top))
                when(sent, left, s1.at[other, c])

        @pl.when(passes_on)
        def _():
            for other in range(h_n):
                for c in range(2):
                    sent = other != h if other or c else all_of(other != h, y > 0)
                    when(sent, left, s2.at[other, c])

    for copy, there in sends[:-1]:
        when(there, copy.wait_send)
    when(no(top), up.wait_send)
    when(all_of(all_of(core == 0, no(top)), no(to_leader)), down_again.wait_send)
    when(all_of(beside_leader, no(bottom)), down_beside.wait_send)
    when(all_of(all_of(core == 0, no(bottom)), member), up_again.wait_send)


def solution(mesh):
    sizes = (mesh.shape["tm"], mesh.shape["height"])

    def on_device(features, gain, shift, weight, bias):
        frames, rows, cols, channels = features.shape
        cout = weight.shape[-1]
        y_n, h_n = sizes[0] // 2, sizes[1]
        any_space = pl.BlockSpec(memory_space=pl.ANY)
        slab = (2 * frames, rows + 2, cols, channels)
        dma = pltpu.SemaphoreType.DMA
        return pl.pallas_call(
            functools.partial(kernel, sizes),
            out_shape=pltpu.VMEM((frames, rows, cols, cout), jnp.bfloat16),
            in_specs=[any_space] * 5,
            out_specs=pl.BlockSpec(memory_space=pltpu.VMEM),
            scratch_shapes=[
                pltpu.VMEM(slab, jnp.bfloat16),
                pltpu.VMEM((4, 2 * frames, 2, cols, channels), jnp.bfloat16),
                pltpu.VMEM(weight.shape, jnp.bfloat16),
                pltpu.VMEM((3, 2, 3, channels, cout), jnp.bfloat16),
                pltpu.VMEM((3, 2, frames * 2 * cols, cout), jnp.float32),
                pltpu.VMEM((2 * frames, cols, channels), jnp.float32),
                pltpu.VMEM((channels,), jnp.float32),
                pltpu.VMEM((channels,), jnp.float32),
                pltpu.VMEM((cout,), jnp.float32),
                *[pltpu.VMEM((8, 128), jnp.float32)] * 5,
                pltpu.VMEM((2 * h_n - 1 + y_n - 1, 8, 128), jnp.float32),
                pltpu.VMEM((y_n, 2, 8, 128), jnp.float32),
                pltpu.VMEM((h_n, 8, 128), jnp.float32),
                dma((frames, rows)), dma((3,)), dma, dma, dma, dma((y_n, 2)), dma((y_n, 2)),
                dma((h_n, 2)), dma((h_n,)), dma((y_n,)), dma, dma((5,)), dma((5,)),
                pltpu.SemaphoreType.REGULAR, pltpu.SemaphoreType.REGULAR((h_n,)),
            ],
            compiler_params=pltpu.CompilerParams(
                collective_id=0, has_side_effects=True, vmem_limit_bytes=60 * 1024 * 1024
            ),
        )(features, gain, shift, weight, bias)

    return jax.shard_map(
        on_device,
        mesh=mesh,
        in_specs=(P(("clips", "tm"), "height", None, None), P(), P(), P(), P()),
        out_specs=P(("clips", "tm"), "height", None, None),
        check_vma=False,
    )
```

```python
import functools

import jax
import jax.numpy as jnp
from jax import lax
from jax.experimental import pallas as pl
from jax.experimental.pallas import tpu as pltpu
from jax.sharding import PartitionSpec as P

MESH = pl.DeviceIdType.MESH
GROUPS = 32
EPSILON = 1e-06


def kernel(sizes, feat, gain, shift, weight, bias, out, raw, act, wbuf, mixed, sums, kept, gbuf, hbuf, bbuf,
           mine, pair, row, row2, late, span, got1, got2, in_sem, small_sem, w_sem, s0, r0, s1, r1, s2, r2, s4, s5, hs, hr, perm0, perm2):
    tm_n, h_n = sizes
    y_n = tm_n // 2
    frames, rows, cols, channels = feat.shape
    loads = {}
    for f in range(frames):
        for r in range(rows):
            loads[f, r] = pltpu.make_async_copy(feat.at[f, r], raw.at[frames + f, 1 + r], in_sem.at[f, r])
            loads[f, r].start()
    smalls = [pltpu.make_async_copy(a, b, small_sem.at[i])
              for i, (a, b) in enumerate(((gain, gbuf), (shift, hbuf), (bias, bbuf)))]
    for copy in smalls:
        copy.start()
    weights = pltpu.make_async_copy(weight, wbuf, w_sem)

    lanes = 128
    parts = channels // lanes
    tm = lax.axis_index("tm")
    h = lax.axis_index("height")
    core = lax.rem(tm, 2)
    y = lax.div(tm, 2)
    first, last = tm == 0, tm == tm_n - 1
    top, bottom = h == 0, h == h_n - 1

    wide = 2 * h_n
    leader = jnp.logical_and(first, top)
    member = jnp.logical_not(leader)
    all_of, any_of, no = jnp.logical_and, jnp.logical_or, jnp.logical_not
    beside_leader = all_of(tm == 1, top)
    passes_on = any_of(all_of(core == 0, member), beside_leader)
    receives_along = all_of(core == 0, no(first))
    to_leader = all_of(first, h == 1)

    def at(dtm, dh):
        return {"tm": tm + dtm, "height": h + dh}

    def in_row(other, c, chip=y):
        return {"tm": chip * 2 + c, "height": other}

    def column(other, c):
        return {"tm": other * 2 + c, "height": h}

    def turn(v):
        half = h_n // 2
        if isinstance(v, int):
            return v if v < half else half + h_n - 1 - v
        return jnp.where(v < half, v, half + h_n - 1 - v)

    here_turn = turn(h)
    def when(condition, f, *args):
        pl.when(condition)(functools.partial(f, *args))

    def signal(sem, device):
        pl.semaphore_signal(sem, inc=1, device_id=device, device_id_type=MESH)

    def send(src, dst, s, r, device):
        return pltpu.make_async_remote_copy(src_ref=src, dst_ref=dst, send_sem=s, recv_sem=r,
                                            device_id=device, device_id_type=MESH)

    barrier = pltpu.get_barrier_semaphore()

    @pl.when(member)
    def _():
        for other in range(1, h_n):
            @pl.when(turn(other) > here_turn)
            def _():
                signal(barrier, in_row(other, 0))
                signal(barrier, in_row(other, 1))
        when(no(beside_leader), signal, barrier, column(y, 1 - core))
        when(no(top), signal, barrier, at(0, -1))
        when(no(bottom), signal, barrier, at(0, 1))

        @pl.when(receives_along)
        def _():
            signal(barrier, at(-1, 0))
            when(no(top), signal, barrier, at(-1, -1))
            when(no(bottom), signal, barrier, at(-1, 1))

        when(any_of(y == 0, all_of(core == 0, top)), signal, barrier, {"tm": 0, "height": 0})
        for other in range(1, y_n):
            @pl.when(other > y)
            def _():
                signal(barrier, column(other, 0))
                signal(barrier, column(other, 1))

    def number(condition):
        return condition.astype(jnp.int32)

    above_it = 2 * y - number(all_of(top, y > 0)) + 1 - number(beside_leader)
    before_it = 2 * here_turn - number(all_of(y == 0, h > 0))
    edges = number(no(bottom)) + number(no(top)) - number(to_leader)
    onward = number(all_of(core == 1, no(last))) * (3 - number(top) - number(bottom))
    for_leader = (wide - 1) + (y_n - 1) + 1
    def edge(src_row, dst_row, frame, dtm, dh, i):
        return send(raw.at[frames:, src_row], raw.at[pl.ds(frame, frames), dst_row],
                    hs.at[i], hr.at[i], at(dtm, dh))

    down = edge(rows, 0, frames, 0, 1, 0)
    up = edge(1, rows + 1, frames, 0, -1, 1)
    down_next = edge(rows, 0, 0, 1, 1, 2)
    up_next = edge(1, rows + 1, 0, 1, -1, 3)
    along = send(raw.at[frames:, 1:rows], raw.at[:frames, 1:rows], hs.at[4], hr.at[4], at(1, 0))
    along_edge = send(raw.at[frames:, rows], raw.at[:frames, rows], hs.at[5], hr.at[5], at(1, 0))
    down_again = edge(0, 0, 0, 1, 0, 2)
    up_again = edge(rows + 1, rows + 1, 0, 1, 0, 3)
    down_beside = send(raw.at[:frames, rows], raw.at[:frames, 0], s5, hr.at[2], at(0, 1))
    total = jnp.zeros((8, channels), jnp.float32)
    squares = jnp.zeros((8, channels), jnp.float32)
    for f, r in loads:
        loads[f, r].wait()
        x = raw[frames + f, 1 + r].astype(jnp.float32).reshape(cols // 8, 8, channels)
        total = total + jnp.sum(x, axis=0)
        squares = squares + jnp.sum(x * x, axis=0)
    weights.start()
    total = jnp.sum(total, axis=0, keepdims=True)
    squares = jnp.sum(squares, axis=0, keepdims=True)
    for k in range(parts):
        mine[k : k + 1, :] = total[:, k * lanes : (k + 1) * lanes]
        mine[parts + k : parts + k + 1, :] = squares[:, k * lanes : (k + 1) * lanes]

    pl.semaphore_wait(barrier, jnp.where(leader, for_leader, above_it + before_it + edges + onward))

    def give(other, c):
        send(mine, got1.at[y, core], s1.at[other, c], r1.at[y, core], column(other, c)).start()

    @pl.when(member)
    def _():
        for other in range(y_n - 1):
            @pl.when(other < y)
            def _():
                if other:
                    give(other, 0)
                else:
                    when(no(top), give, other, 0)
                give(other, 1)
        when(no(beside_leader), give, y, 1 - core)

    sends = (
        (down, no(bottom)),
        (along_edge, no(last)),
        (along, no(last)),
        (down_next, all_of(core == 1, no(any_of(bottom, last)))),
        (up_next, any_of(to_leader, all_of(core == 1, no(any_of(top, last))))),
        (up, all_of(no(top), no(to_leader))),
    )
    along_ends = all_of(no(first), any_of(no(beside_leader), bottom))
    arrivals = (
        (down, no(top)),
        (up, no(bottom)),
        (along, no(first)),
        (down_next, no(any_of(top, first))),
        (up_next, no(any_of(bottom, first))),
    )

    def tell(device):
        return send(mine, late, s0, r0, device)

    @pl.when(leader)
    def _():
        for q in sorted(range(h_n), key=lambda q: -min(q, h_n - q)):
            for c in range(2):
                if q or c:
                    tell(in_row(q, c, 0)).start()
        along_edge.start()
        along.start()
        down.start()
        signal(perm0, {"tm": 0, "height": 1})
        signal(perm0, {"tm": 1, "height": 0})

    def hand_on():
        when(no(top), down.wait_recv)
        when(all_of(all_of(core == 0, no(top)), no(to_leader)), down_again.start)

    def hand_on_up():
        when(no(bottom), up.wait_recv)
        when(all_of(all_of(core == 0, no(bottom)), member), up_again.start)

    @pl.when(member)
    def _():
        for other in range(h_n):
            sender = jnp.where(y == 0, 1, 0) if other == 0 else 0
            when(turn(other) < here_turn, signal, perm2.at[h], in_row(other, sender))

    @pl.when(member)
    def _():
        for copy, there in sends:
            when(there, copy.start)

    @pl.when(leader)
    def _():
        for other in range(1, y_n):
            tell(column(other, 0)).start()

    @pl.when(member)
    def _():
        def arrived(other, c):
            send(mine, mine, s1.at[0, 0], r1.at[other, c], at(0, 0)).wait_recv()

        when(beside_leader, got1.at[0, 0].__setitem__, Ellipsis, jnp.zeros_like(mine))
        when(no(beside_leader), arrived, y, 1 - core)
        pair[...] = mine[...] + got1[y, 1 - core]
        row[...] = pair[...]
        for other in range(1, y_n):
            @pl.when(other > y)
            def _():
                arrived(other, 0)
                arrived(other, 1)
                row[...] += got1[other, 0] + got1[other, 1]

                @pl.when(passes_on)
                def _():
                    for c in range(2):
                        send(pair, got1.at[y, 0], s1.at[other, c], r1.at[y, 0], column(other, c)).start()

        for other in range(y_n):
            @pl.when(other < y)
            def _():
                arrived(other, 0)
                row[...] += got1[other, 0]

        def pass_on(other, c):
            send(row, got2.at[h], s2.at[other, c], r2.at[h], in_row(other, c)).start()

        got2[h] = row[...]

        @pl.when(passes_on)
        def _():
            for other in sorted(range(h_n), key=turn):
                @pl.when(other != h)
                def _():
                    when(turn(other) > here_turn, pl.semaphore_wait, perm2.at[other], 2)
                    if other:
                        pass_on(other, 0)
                    else:
                        when(y > 0, pass_on, other, 0)
                    pass_on(other, 1)

        when(no(to_leader), hand_on)
        hand_on_up()

    weights.wait()

    @pl.loop(0, 9)
    def _(i):
        a, c = i // 3, lax.rem(i, 3)
        for k in range(0, channels, 64):
            g0, g1, g2 = (wbuf[a, b, c, k : k + 64].astype(jnp.float32) for b in range(3))
            even, odd = 0.5 * (g0 + g2), 0.5 * g1
            mixed[a, 0, c, k : k + 64] = (even + odd).astype(jnp.bfloat16)
            mixed[a, 1, c, k : k + 64] = (even - odd).astype(jnp.bfloat16)

    @pl.when(member)
    def _():
        @pl.when(to_leader)
        def _():
            pl.semaphore_wait(perm0, 1)
            up.start()

        @pl.when(all_of(beside_leader, no(bottom)))
        def _():
            along_edge.wait_recv()
            down_beside.start()

        for other in range(h_n):
            when(other != h, send(row, got2.at[other], s2.at[0, 0], r2.at[other], at(0, 0)).wait_recv)
        here = got2[0]
        for other in range(1, h_n):
            here = here + got2[other]
        row2[...] = here

        @pl.when(beside_leader)
        def _():
            pl.semaphore_wait(perm0, 1)
            send(row2, late, s0, r0, {"tm": 0, "height": 0}).start()

    @pl.when(leader)
    def _():
        row2[...] = mine[...]

    relays = all_of(member, y == 0)
    tell(at(0, 0)).wait_recv()

    @pl.when(relays)
    def _():
        for other in range(1, y_n):
            send(late, late, s4.at[other], r0, column(other, core)).start()

    for copy in smalls:
        copy.wait()
    when(leader, hand_on_up)
    when(arrivals[4][1], up_next.wait_recv)
    here = row2[...] + late[...]

    per_group = channels // GROUPS
    high = here.astype(jnp.bfloat16)
    rest = here - high.astype(jnp.float32)
    middle = rest.astype(jnp.bfloat16)
    low = (rest - middle.astype(jnp.float32)).astype(jnp.bfloat16)
    same = (lax.broadcasted_iota(jnp.int32, (lanes, lanes), 0) // per_group
            == lax.broadcasted_iota(jnp.int32, (lanes, lanes), 1) // per_group)
    same = jnp.where(same, 1.0, 0.0).astype(jnp.bfloat16)
    spread = sum(jnp.dot(a, same, preferred_element_type=jnp.float32) for a in (low, middle, high))
    cells = tm_n * h_n * frames * rows * cols * per_group
    spread = spread * (1.0 / cells)
    mean = spread[:parts]
    var = jnp.maximum(spread[parts:] - mean * mean, 0.0)
    scale = lax.rsqrt(var + EPSILON)

    def flat(a):
        return jnp.concatenate([a[k : k + 1] for k in range(parts)], axis=1)

    half_scale = flat(scale) * gbuf[...].reshape(1, channels) * 0.5
    half_shift = hbuf[...].reshape(1, channels) * 0.5 - flat(mean) * half_scale

    step = 16

    def activated(f, r, k):
        source = jnp.where(first, frames, f) if f < frames else f
        v = raw[source, r, k : k + step].astype(jnp.float32) * half_scale + half_shift
        return v + v * jnp.tanh(v)

    def put(p, f, pair, k, value):
        act[p, f, pair, k : k + step] = value.astype(jnp.bfloat16)

    def prepare(f):
        for k in range(0, cols, step):
            d = [activated(f, r, k) for r in range(1, rows + 1)]
            for pair in range(2):
                put(1, f, pair, k, d[2 * pair] + d[2 * pair + 1])
                put(2, f, pair, k, d[2 * pair + 1] - d[2 * pair])
            put(0, f, 1, k, d[1] - d[3])
            kept[f, k : k + step] = d[1]
            put(3, f, 0, k, d[0] - d[2])
            below = jnp.where(bottom, 0.0, activated(f, rows + 1, k))
            put(3, f, 1, k, d[2] - below)

    for f in range(frames, 2 * frames):
        prepare(f)

    m = frames * 2 * cols

    def product(p, c, taps=(0, 1, 2)):
        acc = None
        for a in taps:
            lhs = act[p, a : a + frames].reshape(m, channels)
            rhs = wbuf[a, 2 * (p // 3), c] if p in (0, 3) else mixed[a, p - 1, c]
            part = jnp.dot(lhs, rhs, preferred_element_type=jnp.float32)
            acc = part if acc is None else acc + part
        return acc

    for c in range(3):
        m1, m2 = product(1, c, (2,)), product(2, c, (2,))
        sums[c, 0] = m1 + m2
        sums[c, 1] = m1 - m2

    when(no(first), along.wait_recv)
    when(along_ends, along_edge.wait_recv)
    for f in range(frames):
        prepare(f)
    for c in range(3):
        m1, m2 = product(1, c, (0, 1)), product(2, c, (0, 1))
        sums[c, 0] = sums[c, 0] + (m1 + m2)
        sums[c, 1] = sums[c, 1] + (m1 - m2)

    when(to_leader, hand_on)
    when(arrivals[3][1], down_next.wait_recv)

    for f in range(2 * frames):
        for k in range(0, cols, step):
            above = jnp.where(top, 0.0, activated(f, 0, k))
            put(0, f, 0, k, above - kept[f, k : k + step])

    offset = bbuf[...].reshape(1, -1)
    for c in range(3):
        sums[c, 1] = sums[c, 1] - product(3, c)
        sums[c, 0] = sums[c, 0] + product(0, c)
    for odd in range(2):
        for f in range(frames):
            for pair in range(2):
                at0 = (f * 2 + pair) * cols
                left, middle, right = (sums[c, odd, at0 : at0 + cols] for c in range(3))
                zero = jnp.zeros_like(left[:1])
                left = jnp.concatenate([zero, left[:-1]], axis=0)
                right = jnp.concatenate([right[1:], zero], axis=0)
                out[f, 2 * pair + odd] = (middle + left + right + offset).astype(jnp.bfloat16)

    @pl.when(leader)
    def _():
        send(span, span, s0, r0, at(0, 0)).wait_send()

    @pl.when(relays)
    def _():
        for other in range(1, y_n):
            send(late, late, s4.at[other], r0, at(0, 0)).wait_send()

    when(beside_leader, send(row2, late, s0, r0, at(0, 0)).wait_send)

    @pl.when(member)
    def _():
        def left(sem):
            send(mine, mine, sem, r0, at(0, 0)).wait_send()

        when(no(beside_leader), left, s1.at[y, 1 - core])
        for other in range(y_n):
            for c in range(2):
                sent = any_of(other < y, all_of(other > y, passes_on))
                if not other and not c:
                    sent = all_of(sent, no(top))
                when(sent, left, s1.at[other, c])

        @pl.when(passes_on)
        def _():
            for other in range(h_n):
                for c in range(2):
                    sent = other != h if other or c else all_of(other != h, y > 0)
                    when(sent, left, s2.at[other, c])

    for copy, there in sends[:-1]:
        when(there, copy.wait_send)
    when(no(top), up.wait_send)
    when(all_of(all_of(core == 0, no(top)), no(to_leader)), down_again.wait_send)
    when(all_of(beside_leader, no(bottom)), down_beside.wait_send)
    when(all_of(all_of(core == 0, no(bottom)), member), up_again.wait_send)


def solution(mesh):
    sizes = (mesh.shape["tm"], mesh.shape["height"])

    def on_device(features, gain, shift, weight, bias):
        frames, rows, cols, channels = features.shape
        cout = weight.shape[-1]
        y_n, h_n = sizes[0] // 2, sizes[1]
        any_space = pl.BlockSpec(memory_space=pl.ANY)
        slab = (2 * frames, rows + 2, cols, channels)
        dma = pltpu.SemaphoreType.DMA
        return pl.pallas_call(
            functools.partial(kernel, sizes),
            out_shape=pltpu.VMEM((frames, rows, cols, cout), jnp.bfloat16),
            in_specs=[any_space] * 5,
            out_specs=pl.BlockSpec(memory_space=pltpu.VMEM),
            scratch_shapes=[
                pltpu.VMEM(slab, jnp.bfloat16),
                pltpu.VMEM((4, 2 * frames, 2, cols, channels), jnp.bfloat16),
                pltpu.VMEM(weight.shape, jnp.bfloat16),
                pltpu.VMEM((3, 2, 3, channels, cout), jnp.bfloat16),
                pltpu.VMEM((3, 2, frames * 2 * cols, cout), jnp.float32),
                pltpu.VMEM((2 * frames, cols, channels), jnp.float32),
                pltpu.VMEM((channels,), jnp.float32),
                pltpu.VMEM((channels,), jnp.float32),
                pltpu.VMEM((cout,), jnp.float32),
                *[pltpu.VMEM((8, 128), jnp.float32)] * 5,
                pltpu.VMEM((2 * h_n - 1 + y_n - 1, 8, 128), jnp.float32),
                pltpu.VMEM((y_n, 2, 8, 128), jnp.float32),
                pltpu.VMEM((h_n, 8, 128), jnp.float32),
                dma((frames, rows)), dma((3,)), dma, dma, dma, dma((y_n, 2)), dma((y_n, 2)),
                dma((h_n, 2)), dma((h_n,)), dma((y_n,)), dma, dma((6,)), dma((6,)),
                pltpu.SemaphoreType.REGULAR, pltpu.SemaphoreType.REGULAR((h_n,)),
            ],
            compiler_params=pltpu.CompilerParams(
                collective_id=0, has_side_effects=True, vmem_limit_bytes=60 * 1024 * 1024
            ),
        )(features, gain, shift, weight, bias)

    return jax.shard_map(
        on_device,
        mesh=mesh,
        in_specs=(P(("clips", "tm"), "height", None, None), P(), P(), P(), P()),
        out_specs=P(("clips", "tm"), "height", None, None),
        check_vma=False,
    )
```
